64 devices in a mesh: dp: 4 (over x, y), ep: 16 (over z, core).
Axes of the slice: x: 2, y: 2, z: 8, core: 2. Of those that a mesh axis runs over, the one named last changes fastest.
The devices are a block of a 4x4x8 slice.
Arguments:
- tokens: bfloat16 [64, 1024, 768], P(('dp', 'ep')), parts along dimension 0
- w_gate: bfloat16 [768, 16], replicated
- expert_ids: int32 [64, 1024, 2], P(('dp', 'ep')), parts along dimension 0
- keep_second: int32 [64, 1024], P(('dp', 'ep')), parts along dimension 0
- w_in: bfloat16 [16, 768, 3072], P('ep')
- w_out: bfloat16 [16, 3072, 768], P('ep')
Outputs:
- output: bfloat16 [64, 1024, 768], P(('dp', 'ep')), parts along dimension 0
There are 4 independent parts. The reference program is written for one: setup_inputs(seed, part) draws one part's arguments, and reference() takes and returns one part's arrays. A program takes and returns all parts, laid end to end along the dimension named above; an argument that names none is the same for every part.
All inputs are finite; a program needn't handle non-finite values.
Results may differ from the reference program's by a relative error of at most 0.001.
Values are sent between devices in bfloat16 or wider.
A program may use at most 768 MiB of HBM per device.

```python
import functools
import jax
import jax.numpy as jnp
from jax import lax

GROUPS = 16
TOKENS = 1024
MODEL_DIM = 768
HIDDEN = 3072
EXPERTS = 16
CAPACITY = 2 * TOKENS // EXPERTS


def draw_routing(route_key):
    k_cover, k_raw, k_shift, k_second, k_keep = jax.random.split(route_key, 5)
    cover_keys = jax.random.split(k_cover, GROUPS)
    cover_ids = jax.vmap(functools.partial(jax.random.permutation, x=EXPERTS))(cover_keys)
    hot_shift = jax.random.randint(k_shift, (), 0, EXPERTS)
    raw_ids = jax.random.randint(k_raw, (GROUPS, TOKENS - EXPERTS), 0, EXPERTS + EXPERTS // 2)
    rest_ids = (raw_ids % EXPERTS + hot_shift) % EXPERTS
    first_ids = jnp.concatenate([cover_ids.astype(jnp.int32), rest_ids.astype(jnp.int32)], axis=1)
    second_ids = (first_ids + jax.random.randint(k_second, (GROUPS, TOKENS), 1, EXPERTS)) % EXPERTS
    keep_second = (jax.random.randint(k_keep, (GROUPS, TOKENS), 0, 10) < 9).astype(jnp.int32)
    expert_ids = jnp.stack([first_ids, second_ids], axis=-1).astype(jnp.int32)
    return expert_ids, keep_second


def setup_inputs(seed: int = 0, part: int = 0) -> dict:
    shared_key, parts_key = jax.random.split(jax.random.key(seed))
    part_key = jax.random.fold_in(parts_key, part)
    k_tokens, k_route = jax.random.split(part_key)
    k_gate, k_in, k_out = jax.random.split(shared_key, 3)
    tokens = jax.random.normal(k_tokens, (GROUPS, TOKENS, MODEL_DIM), jnp.float32).astype(jnp.bfloat16)
    expert_ids, keep_second = draw_routing(k_route)
    w_gate = (jax.random.normal(k_gate, (MODEL_DIM, EXPERTS), jnp.float32) * MODEL_DIM ** -0.5).astype(jnp.bfloat16)
    w_in = (jax.random.normal(k_in, (EXPERTS, MODEL_DIM, HIDDEN), jnp.float32) * MODEL_DIM ** -0.5).astype(jnp.bfloat16)
    w_out = (jax.random.normal(k_out, (EXPERTS, HIDDEN, MODEL_DIM), jnp.float32) * (2.0 / HIDDEN) ** 0.5).astype(jnp.bfloat16)
    return {"tokens": tokens, "w_gate": w_gate, "expert_ids": expert_ids, "keep_second": keep_second, "w_in": w_in, "w_out": w_out}


def group_routing(group_tok, group_ids, group_keep, w_gate):
    logits = jnp.dot(group_tok, w_gate, preferred_element_type=jnp.float32)
    gate_probs = jax.nn.softmax(logits, axis=-1)
    first_hot = jax.nn.one_hot(group_ids[:, 0], EXPERTS, dtype=jnp.int32)
    second_hot = jax.nn.one_hot(group_ids[:, 1], EXPERTS, dtype=jnp.int32) * group_keep[:, None]
    gate_first = jnp.sum(gate_probs * first_hot, axis=-1)
    gate_second = jnp.sum(gate_probs * second_hot, axis=-1)
    gate_total = gate_first + gate_second
    gate_first = gate_first / gate_total
    gate_second = gate_second / gate_total
    pos_first = jnp.sum((jnp.cumsum(first_hot, axis=0) - first_hot) * first_hot, axis=-1)
    second_base = jnp.cumsum(second_hot, axis=0) - second_hot + jnp.sum(first_hot, axis=0)[None, :]
    pos_second = jnp.sum(second_base * second_hot, axis=-1)
    slot_first = first_hot[:, :, None] * jax.nn.one_hot(pos_first, CAPACITY, dtype=jnp.float32)[:, None, :]
    slot_second = second_hot[:, :, None] * jax.nn.one_hot(pos_second, CAPACITY, dtype=jnp.float32)[:, None, :]
    dispatch = slot_first + slot_second
    combine = (gate_first[:, None, None] * slot_first + gate_second[:, None, None] * slot_second).astype(jnp.bfloat16)
    return dispatch, combine


def reference(tokens, w_gate, expert_ids, keep_second, w_in, w_out):
    def dispatch_group(operands):
        group_tok, group_ids, group_keep = operands
        dispatch, _ = group_routing(group_tok, group_ids, group_keep, w_gate)
        sent_rows = jnp.einsum("sec,sm->ecm", dispatch.astype(jnp.float32), group_tok.astype(jnp.float32))
        return sent_rows.astype(jnp.bfloat16)

    expert_in = lax.map(dispatch_group, (tokens, expert_ids, keep_second))
    expert_in = jnp.transpose(expert_in, (1, 0, 2, 3))

    def expert_ffn(operands):
        rows_in, w_first, w_second = operands
        flat_rows = rows_in.reshape(GROUPS * CAPACITY, MODEL_DIM)
        hidden = jax.nn.relu(jnp.dot(flat_rows, w_first, preferred_element_type=jnp.float32)).astype(jnp.bfloat16)
        rows_out = jnp.dot(hidden, w_second, preferred_element_type=jnp.float32).astype(jnp.bfloat16)
        return rows_out.reshape(GROUPS, CAPACITY, MODEL_DIM)

    expert_out = lax.map(expert_ffn, (expert_in, w_in, w_out))
    expert_out = jnp.transpose(expert_out, (1, 0, 2, 3))

    def combine_group(operands):
        group_tok, group_ids, group_keep, rows_back = operands
        _, combine = group_routing(group_tok, group_ids, group_keep, w_gate)
        mixed_rows = jnp.einsum("sec,ecm->sm", combine.astype(jnp.float32), rows_back.astype(jnp.float32))
        return mixed_rows.astype(jnp.bfloat16)

    return lax.map(combine_group, (tokens, expert_ids, keep_second, expert_out))
```

```python
import functools

import jax
import jax.numpy as jnp
from jax import lax
from jax.experimental import pallas as pl
from jax.experimental.pallas import tpu as pltpu
from jax.sharding import PartitionSpec as P

MESH = pl.DeviceIdType.MESH
CORES = 2
LANES = 128


def route_slots(ids_ref, keep_ref, experts, capacity):
    tokens = ids_ref.shape[1]
    first = ids_ref[0:1, :]
    second = ids_ref[1:2, :]
    keep = keep_ref[0:1, :]
    expert_row = lax.broadcasted_iota(jnp.int32, (experts, tokens), 0)
    first_hot = jnp.where(expert_row == first, 1.0, 0.0)
    second_hot = jnp.where((expert_row == second) & (keep == 1), 1.0, 0.0)
    hot = jnp.concatenate([first_hot, second_hot], axis=0)
    blocks = tokens // LANES
    stacked = jnp.concatenate([hot[:, b * LANES:(b + 1) * LANES] for b in range(blocks)], axis=0).astype(jnp.bfloat16)
    row = lax.broadcasted_iota(jnp.int32, (LANES, 2 * LANES), 0)
    col = lax.broadcasted_iota(jnp.int32, (LANES, 2 * LANES), 1)
    before = jnp.where((row < col) | (col >= LANES), 1.0, 0.0).astype(jnp.bfloat16)
    counts = jnp.dot(stacked, before, preferred_element_type=jnp.float32)
    rows = 2 * experts
    offset = jnp.zeros((rows, LANES), jnp.float32)
    prefix = []
    for b in range(blocks):
        part = counts[b * rows:(b + 1) * rows]
        prefix.append(part[:, :LANES] + offset)
        offset = offset + part[:, LANES:]
    first_total = offset[:experts]
    slot_first, slot_second = [], []
    for b in range(blocks):
        lanes = slice(b * LANES, (b + 1) * LANES)
        pos_first = jnp.sum(prefix[b][:experts] * first_hot[:, lanes], axis=0, keepdims=True)
        pos_second = jnp.sum((prefix[b][experts:] + first_total) * second_hot[:, lanes], axis=0, keepdims=True)
        slot_first.append(pos_first)
        slot_second.append(pos_second)
    pos_first = jnp.concatenate(slot_first, axis=1).astype(jnp.int32)
    pos_second = jnp.concatenate(slot_second, axis=1).astype(jnp.int32)
    slot_first = jnp.where(pos_first < capacity, first * capacity + pos_first, -1)
    slot_second = jnp.where((keep == 1) & (pos_second < capacity), second * capacity + pos_second, -1)
    return slot_first, slot_second, first_hot, second_hot


def layer_kernel(n, tokens_hbm, gate_ref, ids_ref, keep_ref, w_in_hbm, w_out_hbm, out_ref,
                 tokens_ref, w_in, w_out, send, recv, back, ret, hidden, combine, total, slots,
                 load_sem, send_sem, recv_sem, back_sem, ret_sem):
    me = lax.axis_index("ep")
    part = lax.axis_index("dp")
    chips = n // CORES
    chip = me // CORES
    core = lax.rem(me, CORES)
    experts = gate_ref.shape[0]
    tokens, model = tokens_ref.shape
    hid = w_in.shape[1]
    capacity = 2 * tokens // experts
    pair = CORES * capacity
    local = chips - 1

    load_tokens = pltpu.make_async_copy(tokens_hbm, tokens_ref, load_sem.at[0])
    load_in = pltpu.make_async_copy(w_in_hbm, w_in, load_sem.at[1])
    load_out = pltpu.make_async_copy(w_out_hbm, w_out, load_sem.at[2])
    load_tokens.start()
    load_in.start()
    load_out.start()

    barrier = pltpu.get_barrier_semaphore()
    for k in range(1, n):
        pl.semaphore_signal(barrier, inc=1, device_id=(part, lax.rem(me + k, n)), device_id_type=MESH)

    slot_first, slot_second, first_hot, second_hot = route_slots(ids_ref, keep_ref, experts, capacity)
    slots[0:1, :] = slot_first
    slots[1:2, :] = slot_second

    def offset_of(step):
        size = (chips - step) // 2
        return jnp.where(lax.rem(step, 2) == 1, size, chips - size)

    def target_chip(step):
        return lax.rem(chip + offset_of(step), chips)

    def source_chip(step):
        return lax.rem(chip + chips - offset_of(step), chips)

    def forward(step, c):
        return pltpu.make_async_remote_copy(
            src_ref=send.at[step, c], dst_ref=recv.at[step, core],
            send_sem=send_sem.at[step, c], recv_sem=recv_sem.at[step, core],
            device_id=(part, target_chip(step) * CORES + c), device_id_type=MESH)

    def arrived(step, c):
        return pltpu.make_async_remote_copy(
            src_ref=send.at[step, c], dst_ref=recv.at[step, c],
            send_sem=send_sem.at[step, c], recv_sem=recv_sem.at[step, c],
            device_id=(part, target_chip(step) * CORES + c), device_id_type=MESH)

    def reply(step, c):
        return pltpu.make_async_remote_copy(
            src_ref=back.at[step, c], dst_ref=ret.at[step, core],
            send_sem=back_sem.at[step, c], recv_sem=ret_sem.at[step, core],
            device_id=(part, source_chip(step) * CORES + c), device_id_type=MESH)

    def returned(step, c):
        return pltpu.make_async_remote_copy(
            src_ref=back.at[step, c], dst_ref=ret.at[step, c],
            send_sem=back_sem.at[step, c], recv_sem=ret_sem.at[step, c],
            device_id=(part, source_chip(step) * CORES + c), device_id_type=MESH)

    slot_row = lax.broadcasted_iota(jnp.int32, (pair, tokens), 0)

    def dispatch(step):
        base = target_chip(step) * pair
        hit = (slot_row == slots[0:1, :] - base) | (slot_row == slots[1:2, :] - base)
        pick = jnp.where(hit, 1.0, 0.0).astype(jnp.bfloat16)
        for c in range(CORES):
            rows = jnp.dot(pick[c * capacity:(c + 1) * capacity], tokens_ref[...], preferred_element_type=jnp.float32)
            send[step, c] = rows.astype(jnp.bfloat16)

    load_tokens.wait()
    dispatch(0)
    pl.semaphore_wait(barrier, n - 1)

    @pl.loop(0, local)
    def _(step):
        for c in range(CORES):
            forward(step, c).start()
        dispatch(step + 1)

    forward(local, 1 - core).start()
    recv[local, core] = send[local, core]

    logits = lax.dot_general(gate_ref[...], tokens_ref[...], (((1,), (1,)), ((), ())), preferred_element_type=jnp.float32)
    shifted = jnp.exp(logits - jnp.max(logits, axis=0, keepdims=True))
    probs = shifted / jnp.sum(shifted, axis=0, keepdims=True)
    gate_first = jnp.sum(probs * first_hot, axis=0, keepdims=True)
    gate_second = jnp.sum(probs * second_hot, axis=0, keepdims=True)
    gate_total = gate_first + gate_second
    gate_first = gate_first / gate_total
    gate_second = gate_second / gate_total

    load_in.wait()
    load_out.wait()

    def experts_on(step):
        rows = recv[step].reshape(pair, model)
        tile = 512
        for t in range(hid // tile):
            cols = slice(t * tile, (t + 1) * tile)
            up = jnp.dot(rows, w_in[:, cols], preferred_element_type=jnp.float32)
            hidden[:, cols] = jnp.maximum(up, 0.0).astype(jnp.bfloat16)
        tile = 256
        for t in range(model // tile):
            cols = slice(t * tile, (t + 1) * tile)
            down = jnp.dot(hidden[...], w_out[:, cols], preferred_element_type=jnp.float32).astype(jnp.bfloat16)
            for c in range(CORES):
                back[step, c, :, cols] = down[c * capacity:(c + 1) * capacity]

    arrived(local, 1 - core).wait_recv()
    experts_on(local)
    reply(local, 1 - core).start()
    ret[local, core] = back[local, core]

    for step in range(chips):
        base = target_chip(step) * pair
        weight = jnp.where(slot_row == slots[0:1, :] - base, gate_first, 0.0) + jnp.where(slot_row == slots[1:2, :] - base, gate_second, 0.0)
        combine[step] = weight.astype(jnp.bfloat16).T

    @pl.loop(0, local)
    def _(step):
        for c in range(CORES):
            arrived(step, c).wait_recv()
        experts_on(step)
        for c in range(CORES):
            reply(step, c).start()

    block = 256

    def mixed(step, r):
        return jnp.dot(combine[step, r * block:(r + 1) * block, :], ret[step].reshape(pair, model), preferred_element_type=jnp.float32)

    returned(local, 1 - core).wait_recv()
    for r in range(tokens // block):
        total[r * block:(r + 1) * block, :] = mixed(local, r)

    @pl.loop(0, local - 1)
    def _(step):
        for c in range(CORES):
            returned(step, c).wait_recv()
        for r in range(tokens // block):
            total[r * block:(r + 1) * block, :] += mixed(step, r)

    for c in range(CORES):
        returned(local - 1, c).wait_recv()
    for r in range(tokens // block):
        rows = slice(r * block, (r + 1) * block)
        out_ref[rows, :] = (total[rows, :] + mixed(local - 1, r)).astype(jnp.bfloat16)

    @pl.loop(0, local)
    def _(step):
        for c in range(CORES):
            forward(step, c).wait_send()
            reply(step, c).wait_send()

    forward(local, 1 - core).wait_send()
    reply(local, 1 - core).wait_send()


def solution(mesh):
    n = mesh.shape["ep"]
    chips = n // CORES

    def local_layer(tokens, w_gate, expert_ids, keep_second, w_in, w_out):
        count, model = tokens.shape[1:]
        experts = w_gate.shape[1]
        hid = w_in.shape[2]
        capacity = 2 * count // experts
        buffer = pltpu.VMEM((chips, CORES, capacity, model), jnp.bfloat16)
        vmem = pl.BlockSpec(memory_space=pltpu.VMEM)
        hbm = pl.BlockSpec(memory_space=pl.ANY)
        out = pl.pallas_call(
            functools.partial(layer_kernel, n),
            out_shape=jax.ShapeDtypeStruct((count, model), jnp.bfloat16),
            in_specs=[hbm, vmem, vmem, vmem, hbm, hbm],
            out_specs=vmem,
            scratch_shapes=[
                pltpu.VMEM((count, model), jnp.bfloat16),
                pltpu.VMEM((model, hid), jnp.bfloat16),
                pltpu.VMEM((hid, model), jnp.bfloat16),
                buffer, buffer, buffer, buffer,
                pltpu.VMEM((CORES * capacity, hid), jnp.bfloat16),
                pltpu.VMEM((chips, count, CORES * capacity), jnp.bfloat16),
                pltpu.VMEM((count, model), jnp.float32),
                pltpu.VMEM((8, count), jnp.int32),
                pltpu.SemaphoreType.DMA((3,)),
                pltpu.SemaphoreType.DMA((chips, CORES)),
                pltpu.SemaphoreType.DMA((chips, CORES)),
                pltpu.SemaphoreType.DMA((chips, CORES)),
                pltpu.SemaphoreType.DMA((chips, CORES)),
            ],
            compiler_params=pltpu.CompilerParams(collective_id=0, has_side_effects=True, vmem_limit_bytes=58 * 2**20),
        )(tokens[0], w_gate.T, expert_ids[0].T, keep_second, w_in[0], w_out[0])
        return out[None]

    group_spec = P(("dp", "ep"))
    return jax.shard_map(local_layer, mesh=mesh, in_specs=(group_spec, P(), group_spec, group_spec, P("ep"), P("ep")), out_specs=group_spec, check_vma=False)
```

```python
import functools

import jax
import jax.numpy as jnp
from jax import lax
from jax.experimental import pallas as pl
from jax.experimental.pallas import tpu as pltpu
from jax.sharding import PartitionSpec as P

MESH = pl.DeviceIdType.MESH
CORES = 2
LANES = 128


def route_slots(ids_ref, keep_ref, experts, capacity):
    tokens = ids_ref.shape[1]
    first = ids_ref[0:1, :]
    second = ids_ref[1:2, :]
    keep = keep_ref[0:1, :]
    expert_row = lax.broadcasted_iota(jnp.int32, (experts, tokens), 0)
    first_hot = jnp.where(expert_row == first, 1.0, 0.0)
    second_hot = jnp.where((expert_row == second) & (keep == 1), 1.0, 0.0)
    hot = jnp.concatenate([first_hot, second_hot], axis=0)
    blocks = tokens // LANES
    stacked = jnp.concatenate([hot[:, b * LANES:(b + 1) * LANES] for b in range(blocks)], axis=0).astype(jnp.bfloat16)
    row = lax.broadcasted_iota(jnp.int32, (LANES, 2 * LANES), 0)
    col = lax.broadcasted_iota(jnp.int32, (LANES, 2 * LANES), 1)
    before = jnp.where((row < col) | (col >= LANES), 1.0, 0.0).astype(jnp.bfloat16)
    counts = jnp.dot(stacked, before, preferred_element_type=jnp.float32)
    rows = 2 * experts
    offset = jnp.zeros((rows, LANES), jnp.float32)
    prefix = []
    for b in range(blocks):
        part = counts[b * rows:(b + 1) * rows]
        prefix.append(part[:, :LANES] + offset)
        offset = offset + part[:, LANES:]
    first_total = offset[:experts]
    slot_first, slot_second = [], []
    for b in range(blocks):
        lanes = slice(b * LANES, (b + 1) * LANES)
        pos_first = jnp.sum(prefix[b][:experts] * first_hot[:, lanes], axis=0, keepdims=True)
        pos_second = jnp.sum((prefix[b][experts:] + first_total) * second_hot[:, lanes], axis=0, keepdims=True)
        slot_first.append(pos_first)
        slot_second.append(pos_second)
    pos_first = jnp.concatenate(slot_first, axis=1).astype(jnp.int32)
    pos_second = jnp.concatenate(slot_second, axis=1).astype(jnp.int32)
    slot_first = jnp.where(pos_first < capacity, first * capacity + pos_first, -1)
    slot_second = jnp.where((keep == 1) & (pos_second < capacity), second * capacity + pos_second, -1)
    return slot_first, slot_second, first_hot, second_hot


def layer_kernel(n, tokens_hbm, gate_hbm, ids_hbm, keep_hbm, w_in_hbm, w_out_hbm, out_ref,
                 tokens_ref, gate_ref, ids_ref, keep_ref, w_in, w_out, send, recv, back, ret, hidden, combine, total, slots,
                 load_sem, send_sem, recv_sem, back_sem, ret_sem):
    me = lax.axis_index("ep")
    part = lax.axis_index("dp")
    chips = n // CORES
    chip = me // CORES
    core = lax.rem(me, CORES)
    experts = gate_ref.shape[0]
    tokens, model = tokens_ref.shape
    hid = w_in.shape[1]
    capacity = 2 * tokens // experts
    pair = CORES * capacity
    local = chips - 1

    load_ids = pltpu.make_async_copy(ids_hbm, ids_ref, load_sem.at[3])
    load_keep = pltpu.make_async_copy(keep_hbm, keep_ref, load_sem.at[4])
    load_gate = pltpu.make_async_copy(gate_hbm, gate_ref, load_sem.at[5])
    load_tokens = pltpu.make_async_copy(tokens_hbm, tokens_ref, load_sem.at[0])
    load_in = pltpu.make_async_copy(w_in_hbm, w_in, load_sem.at[1])
    load_out = pltpu.make_async_copy(w_out_hbm, w_out, load_sem.at[2])
    load_ids.start()
    load_keep.start()
    load_tokens.start()
    load_gate.start()

    barrier = pltpu.get_barrier_semaphore()
    for k in range(1, n):
        pl.semaphore_signal(barrier, inc=1, device_id=(part, lax.rem(me + k, n)), device_id_type=MESH)

    load_ids.wait()
    load_keep.wait()
    slot_first, slot_second, first_hot, second_hot = route_slots(ids_ref, keep_ref, experts, capacity)
    slots[0:1, :] = slot_first
    slots[1:2, :] = slot_second

    half = chips // 2
    order = [half - 1, half + 1, half] + [k for d in range(half - 2, 0, -1) for k in (d, chips - d)] + [0]

    def offset_of(step):
        if isinstance(step, int):
            return order[step]
        offset = order[0]
        for index, value in enumerate(order[1:-1], 1):
            offset = jnp.where(step == index, value, offset)
        return offset

    def target_chip(step):
        return lax.rem(chip + offset_of(step), chips)

    def source_chip(step):
        return lax.rem(chip + chips - offset_of(step), chips)

    def forward(step, c):
        return pltpu.make_async_remote_copy(
            src_ref=send.at[step, c], dst_ref=recv.at[step, core],
            send_sem=send_sem.at[step, c], recv_sem=recv_sem.at[step, core],
            device_id=(part, target_chip(step) * CORES + c), device_id_type=MESH)

    def arrived(step, c):
        return pltpu.make_async_remote_copy(
            src_ref=send.at[step, c], dst_ref=recv.at[step, c],
            send_sem=send_sem.at[step, c], recv_sem=recv_sem.at[step, c],
            device_id=(part, target_chip(step) * CORES + c), device_id_type=MESH)

    def reply(step, c):
        return pltpu.make_async_remote_copy(
            src_ref=back.at[step, c], dst_ref=ret.at[step, core],
            send_sem=back_sem.at[step, c], recv_sem=ret_sem.at[step, core],
            device_id=(part, source_chip(step) * CORES + c), device_id_type=MESH)

    def returned(step, c):
        return pltpu.make_async_remote_copy(
            src_ref=back.at[step, c], dst_ref=ret.at[step, c],
            send_sem=back_sem.at[step, c], recv_sem=ret_sem.at[step, c],
            device_id=(part, source_chip(step) * CORES + c), device_id_type=MESH)

    slot_row = lax.broadcasted_iota(jnp.int32, (pair, tokens), 0)

    def dispatch(step):
        base = target_chip(step) * pair
        hit = (slot_row == slots[0:1, :] - base) | (slot_row == slots[1:2, :] - base)
        pick = jnp.where(hit, 1.0, 0.0).astype(jnp.bfloat16)
        rows = jnp.dot(pick, tokens_ref[...], preferred_element_type=jnp.float32).astype(jnp.bfloat16)
        send[step] = rows.reshape(CORES, capacity, model)

    load_tokens.wait()
    load_in.start()
    load_out.start()
    dispatch(0)
    pl.semaphore_wait(barrier, n - 1)
    for step in range(local):
        for c in range(CORES):
            forward(step, c).start()
        dispatch(step + 1)

    forward(local, 1 - core).start()
    recv[local, core] = send[local, core]

    load_gate.wait()
    logits = lax.dot_general(gate_ref[...], tokens_ref[...], (((1,), (1,)), ((), ())), preferred_element_type=jnp.float32)
    shifted = jnp.exp(logits - jnp.max(logits, axis=0, keepdims=True))
    probs = shifted / jnp.sum(shifted, axis=0, keepdims=True)
    gate_first = jnp.sum(probs * first_hot, axis=0, keepdims=True)
    gate_second = jnp.sum(probs * second_hot, axis=0, keepdims=True)
    gate_total = gate_first + gate_second
    gate_first = gate_first / gate_total
    gate_second = gate_second / gate_total

    load_in.wait()
    load_out.wait()

    def experts_on(step):
        rows = recv[step].reshape(pair, model)
        tile = 512
        for t in range(hid // tile):
            cols = slice(t * tile, (t + 1) * tile)
            up = jnp.dot(rows, w_in[:, cols], preferred_element_type=jnp.float32)
            hidden[:, cols] = jnp.maximum(up, 0.0).astype(jnp.bfloat16)
        tile = 256
        for t in range(model // tile):
            cols = slice(t * tile, (t + 1) * tile)
            down = jnp.dot(hidden[...], w_out[:, cols], preferred_element_type=jnp.float32).astype(jnp.bfloat16)
            for c in range(CORES):
                back[step, c, :, cols] = down[c * capacity:(c + 1) * capacity]

    arrived(local, 1 - core).wait_recv()
    experts_on(local)
    reply(local, 1 - core).start()
    ret[local, core] = back[local, core]

    for step in range(chips):
        base = target_chip(step) * pair
        weight = jnp.where(slot_row == slots[0:1, :] - base, gate_first, 0.0) + jnp.where(slot_row == slots[1:2, :] - base, gate_second, 0.0)
        combine[step] = weight.astype(jnp.bfloat16).T

    @pl.loop(0, local)
    def _(step):
        for c in range(CORES):
            arrived(step, c).wait_recv()
        experts_on(step)
        for c in range(CORES):
            reply(step, c).start()

    block = 256

    def mixed(step, r):
        return jnp.dot(combine[step, r * block:(r + 1) * block, :], ret[step].reshape(pair, model), preferred_element_type=jnp.float32)

    returned(local, 1 - core).wait_recv()
    for r in range(tokens // block):
        total[r * block:(r + 1) * block, :] = mixed(local, r)

    @pl.loop(0, local - 1)
    def _(step):
        for c in range(CORES):
            returned(step, c).wait_recv()
        for r in range(tokens // block):
            total[r * block:(r + 1) * block, :] += mixed(step, r)

    for c in range(CORES):
        returned(local - 1, c).wait_recv()
    for r in range(tokens // block):
        rows = slice(r * block, (r + 1) * block)
        out_ref[rows, :] = (total[rows, :] + mixed(local - 1, r)).astype(jnp.bfloat16)

    @pl.loop(0, local)
    def _(step):
        for c in range(CORES):
            forward(step, c).wait_send()
            reply(step, c).wait_send()

    forward(local, 1 - core).wait_send()
    reply(local, 1 - core).wait_send()


def solution(mesh):
    n = mesh.shape["ep"]
    chips = n // CORES

    def local_layer(tokens, w_gate, expert_ids, keep_second, w_in, w_out):
        count, model = tokens.shape[1:]
        experts = w_gate.shape[1]
        hid = w_in.shape[2]
        capacity = 2 * count // experts
        buffer = pltpu.VMEM((chips, CORES, capacity, model), jnp.bfloat16)
        vmem = pl.BlockSpec(memory_space=pltpu.VMEM)
        hbm = pl.BlockSpec(memory_space=pltpu.HBM)
        out = pl.pallas_call(
            functools.partial(layer_kernel, n),
            out_shape=pltpu.VMEM((count, model), jnp.bfloat16),
            in_specs=[hbm] * 6,
            out_specs=vmem,
            scratch_shapes=[
                pltpu.VMEM((count, model), jnp.bfloat16),
                pltpu.VMEM((experts, model), jnp.bfloat16),
                pltpu.VMEM((2, count), jnp.int32),
                pltpu.VMEM((1, count), jnp.int32),
                pltpu.VMEM((model, hid), jnp.bfloat16),
                pltpu.VMEM((hid, model), jnp.bfloat16),
                buffer, buffer, buffer, buffer,
                pltpu.VMEM((CORES * capacity, hid), jnp.bfloat16),
                pltpu.VMEM((chips, count, CORES * capacity), jnp.bfloat16),
                pltpu.VMEM((count, model), jnp.float32),
                pltpu.VMEM((8, count), jnp.int32),
                pltpu.SemaphoreType.DMA((6,)),
                pltpu.SemaphoreType.DMA((chips, CORES)),
                pltpu.SemaphoreType.DMA((chips, CORES)),
                pltpu.SemaphoreType.DMA((chips, CORES)),
                pltpu.SemaphoreType.DMA((chips, CORES)),
            ],
            compiler_params=pltpu.CompilerParams(collective_id=0, has_side_effects=True, vmem_limit_bytes=50 * 2**20),
        )(*(pltpu.with_memory_space_constraint(x, pltpu.HBM) for x in (tokens[0], w_gate.T, expert_ids[0].T, keep_second, w_in[0], w_out[0])))
        return out[None]

    group_spec = P(("dp", "ep"))
    return jax.shard_map(local_layer, mesh=mesh, in_specs=(group_spec, P(), group_spec, group_spec, P("ep"), P("ep")), out_specs=group_spec, check_vma=False)
```

```python
import functools

import jax
import jax.numpy as jnp
from jax import lax
from jax.experimental import pallas as pl
from jax.experimental.pallas import tpu as pltpu
from jax.sharding import PartitionSpec as P

MESH = pl.DeviceIdType.MESH
CORES = 2
LANES = 128


def route_slots(ids_ref, keep_ref, experts, capacity):
    tokens = ids_ref.shape[1]
    first = ids_ref[0:1, :]
    second = ids_ref[1:2, :]
    keep = keep_ref[0:1, :]
    expert_row = lax.broadcasted_iota(jnp.int32, (experts, tokens), 0)
    first_hot = jnp.where(expert_row == first, 1.0, 0.0)
    second_hot = jnp.where((expert_row == second) & (keep == 1), 1.0, 0.0)
    hot = jnp.concatenate([first_hot, second_hot], axis=0)
    blocks = tokens // LANES
    stacked = jnp.concatenate([hot[:, b * LANES:(b + 1) * LANES] for b in range(blocks)], axis=0).astype(jnp.bfloat16)
    row = lax.broadcasted_iota(jnp.int32, (LANES, 2 * LANES), 0)
    col = lax.broadcasted_iota(jnp.int32, (LANES, 2 * LANES), 1)
    before = jnp.where((row < col) | (col >= LANES), 1.0, 0.0).astype(jnp.bfloat16)
    counts = jnp.dot(stacked, before, preferred_element_type=jnp.float32)
    rows = 2 * experts
    offset = jnp.zeros((rows, LANES), jnp.float32)
    prefix = []
    for b in range(blocks):
        part = counts[b * rows:(b + 1) * rows]
        prefix.append(part[:, :LANES] + offset)
        offset = offset + part[:, LANES:]
    first_total = offset[:experts]
    slot_first, slot_second = [], []
    for b in range(blocks):
        lanes = slice(b * LANES, (b + 1) * LANES)
        pos_first = jnp.sum(prefix[b][:experts] * first_hot[:, lanes], axis=0, keepdims=True)
        pos_second = jnp.sum((prefix[b][experts:] + first_total) * second_hot[:, lanes], axis=0, keepdims=True)
        slot_first.append(pos_first)
        slot_second.append(pos_second)
    pos_first = jnp.concatenate(slot_first, axis=1).astype(jnp.int32)
    pos_second = jnp.concatenate(slot_second, axis=1).astype(jnp.int32)
    slot_first = jnp.where(pos_first < capacity, first * capacity + pos_first, -1)
    slot_second = jnp.where((keep == 1) & (pos_second < capacity), second * capacity + pos_second, -1)
    return slot_first, slot_second, first_hot, second_hot


def layer_kernel(n, tokens_hbm, gate_hbm, ids_hbm, keep_hbm, w_in_hbm, w_out_hbm, out_ref,
                 tokens_ref, gate_ref, ids_ref, keep_ref, w_in, w_out, send, recv, back, ret, hidden, combine, total, slots, picks,
                 load_sem, send_sem, recv_sem, back_sem, ret_sem):
    me = lax.axis_index("ep")
    part = lax.axis_index("dp")
    chips = n // CORES
    chip = me // CORES
    core = lax.rem(me, CORES)
    experts = gate_ref.shape[0]
    tokens, model = tokens_ref.shape
    hid = w_in.shape[1]
    capacity = 2 * tokens // experts
    pair = CORES * capacity
    local = chips - 1

    load_ids = pltpu.make_async_copy(ids_hbm, ids_ref, load_sem.at[3])
    load_keep = pltpu.make_async_copy(keep_hbm, keep_ref, load_sem.at[4])
    load_gate = pltpu.make_async_copy(gate_hbm, gate_ref, load_sem.at[5])
    quarter = tokens // 4
    quarters = [slice(k * quarter, (k + 1) * quarter) for k in range(4)]
    load_tokens = [pltpu.make_async_copy(tokens_hbm.at[rows], tokens_ref.at[rows], load_sem.at[6 + k]) for k, rows in enumerate(quarters)]
    load_in = pltpu.make_async_copy(w_in_hbm, w_in, load_sem.at[0])
    load_out = pltpu.make_async_copy(w_out_hbm, w_out, load_sem.at[1])
    load_ids.start()
    load_keep.start()
    for load in load_tokens:
        load.start()
    load_gate.start()

    barrier = pltpu.get_barrier_semaphore()
    for k in range(1, n):
        pl.semaphore_signal(barrier, inc=1, device_id=(part, lax.rem(me + k, n)), device_id_type=MESH)

    load_ids.wait()
    load_keep.wait()
    slot_first, slot_second, first_hot, second_hot = route_slots(ids_ref, keep_ref, experts, capacity)
    slots[0:1, :] = slot_first
    slots[1:2, :] = slot_second

    half = chips // 2
    order = [k for d in range(half - 1, 1, -1) for k in (d, chips - d)] + [half, 1, chips - 1, 0]

    def offset_of(step):
        if isinstance(step, int):
            return order[step]
        offset = order[0]
        for index, value in enumerate(order[1:-1], 1):
            offset = jnp.where(step == index, value, offset)
        return offset

    def target_chip(step):
        return lax.rem(chip + offset_of(step), chips)

    def source_chip(step):
        return lax.rem(chip + chips - offset_of(step), chips)

    def forward(step, c):
        return pltpu.make_async_remote_copy(
            src_ref=send.at[step, c], dst_ref=recv.at[step, core],
            send_sem=send_sem.at[step, c], recv_sem=recv_sem.at[step, core],
            device_id=(part, target_chip(step) * CORES + c), device_id_type=MESH)

    def arrived(step, c):
        return pltpu.make_async_remote_copy(
            src_ref=send.at[step, c], dst_ref=recv.at[step, c],
            send_sem=send_sem.at[step, c], recv_sem=recv_sem.at[step, c],
            device_id=(part, target_chip(step) * CORES + c), device_id_type=MESH)

    def reply(step, c):
        return pltpu.make_async_remote_copy(
            src_ref=back.at[step, c], dst_ref=ret.at[step, core],
            send_sem=back_sem.at[step, c], recv_sem=ret_sem.at[step, core],
            device_id=(part, source_chip(step) * CORES + c), device_id_type=MESH)

    def returned(step, c):
        return pltpu.make_async_remote_copy(
            src_ref=back.at[step, c], dst_ref=ret.at[step, c],
            send_sem=back_sem.at[step, c], recv_sem=ret_sem.at[step, c],
            device_id=(part, source_chip(step) * CORES + c), device_id_type=MESH)

    slot_row = lax.broadcasted_iota(jnp.int32, (pair, tokens), 0)

    def pick_of(step):
        base = target_chip(step) * pair
        hit = (slot_row == slots[0:1, :] - base) | (slot_row == slots[1:2, :] - base)
        return jnp.where(hit, 1.0, 0.0).astype(jnp.bfloat16)

    def keep_rows(step, rows):
        send[step] = rows.astype(jnp.bfloat16).reshape(CORES, capacity, model)

    def start_forward(step):
        for c in (core, 1 - core):
            forward(step, c).start()

    def turn(index):
        mirror = order.index((chips - order[index]) % chips)
        return index

    early = (turn(0), turn(1))
    for k, step in enumerate(early):
        picks[k] = pick_of(step)
    for load, rows in zip(load_tokens[:-1], quarters[:-1]):
        load.wait()
        for k in range(2):
            part_sum = jnp.dot(picks[k, :, rows], tokens_ref[rows, :], preferred_element_type=jnp.float32)
            kept = slice(k * pair, (k + 1) * pair)
            if rows.start == 0:
                total[kept, :] = part_sum
            else:
                total[kept, :] += part_sum
    load_tokens[-1].wait()
    load_in.start()
    load_out.start()
    for k, step in enumerate(early):
        rows = quarters[-1]
        keep_rows(step, total[k * pair:(k + 1) * pair, :] + jnp.dot(picks[k, :, rows], tokens_ref[rows, :], preferred_element_type=jnp.float32))
        if k == 0:
            pl.semaphore_wait(barrier, n - 1)
        start_forward(step)
    for index in range(2, chips):
        step = turn(index)
        keep_rows(step, jnp.dot(pick_of(step), tokens_ref[...], preferred_element_type=jnp.float32))
        if index < local:
            start_forward(step)

    forward(local, 1 - core).start()
    recv[local, core] = send[local, core]

    load_gate.wait()
    logits = lax.dot_general(gate_ref[...], tokens_ref[...], (((1,), (1,)), ((), ())), preferred_element_type=jnp.float32)
    shifted = jnp.exp(logits - jnp.max(logits, axis=0, keepdims=True))
    probs = shifted / jnp.sum(shifted, axis=0, keepdims=True)
    gate_first = jnp.sum(probs * first_hot, axis=0, keepdims=True)
    gate_second = jnp.sum(probs * second_hot, axis=0, keepdims=True)
    gate_total = gate_first + gate_second
    gate_first = gate_first / gate_total
    gate_second = gate_second / gate_total

    load_in.wait()
    load_out.wait()

    def experts_on(step):
        rows = recv[step].reshape(pair, model)
        tile = 512
        for t in range(hid // tile):
            cols = slice(t * tile, (t + 1) * tile)
            up = jnp.dot(rows, w_in[:, cols], preferred_element_type=jnp.float32)
            hidden[:, cols] = jnp.maximum(up, 0.0).astype(jnp.bfloat16)
        tile = 256
        for t in range(model // tile):
            cols = slice(t * tile, (t + 1) * tile)
            down = jnp.dot(hidden[...], w_out[:, cols], preferred_element_type=jnp.float32).astype(jnp.bfloat16)
            for c in range(CORES):
                back[step, c, :, cols] = down[c * capacity:(c + 1) * capacity]

    arrived(local, 1 - core).wait_recv()
    experts_on(local)
    reply(local, 1 - core).start()
    ret[local, core] = back[local, core]

    for step in range(chips):
        base = target_chip(step) * pair
        weight = jnp.where(slot_row == slots[0:1, :] - base, gate_first, 0.0) + jnp.where(slot_row == slots[1:2, :] - base, gate_second, 0.0)
        combine[step] = weight.astype(jnp.bfloat16).T

    @pl.loop(0, local)
    def _(step):
        for c in range(CORES):
            arrived(step, c).wait_recv()
        experts_on(step)
        for c in (1, 0):
            reply(step, c).start()

    block = 256

    def mixed(step, r):
        return jnp.dot(combine[step, r * block:(r + 1) * block, :], ret[step].reshape(pair, model), preferred_element_type=jnp.float32)

    returned(local, 1 - core).wait_recv()
    for r in range(tokens // block):
        total[r * block:(r + 1) * block, :] = mixed(local, r)

    @pl.loop(0, local - 1)
    def _(step):
        for c in range(CORES):
            returned(step, c).wait_recv()
        for r in range(tokens // block):
            total[r * block:(r + 1) * block, :] += mixed(step, r)

    for c in range(CORES):
        returned(local - 1, c).wait_recv()
    for r in range(tokens // block):
        rows = slice(r * block, (r + 1) * block)
        out_ref[rows, :] = (total[rows, :] + mixed(local - 1, r)).astype(jnp.bfloat16)

    @pl.loop(0, local)
    def _(step):
        for c in range(CORES):
            forward(step, c).wait_send()
            reply(step, c).wait_send()

    forward(local, 1 - core).wait_send()
    reply(local, 1 - core).wait_send()


def solution(mesh):
    n = mesh.shape["ep"]
    chips = n // CORES

    def local_layer(tokens, w_gate, expert_ids, keep_second, w_in, w_out):
        count, model = tokens.shape[1:]
        experts = w_gate.shape[1]
        hid = w_in.shape[2]
        capacity = 2 * count // experts
        buffer = pltpu.VMEM((chips, CORES, capacity, model), jnp.bfloat16)
        vmem = pl.BlockSpec(memory_space=pltpu.VMEM)
        hbm = pl.BlockSpec(memory_space=pltpu.HBM)
        out = pl.pallas_call(
            functools.partial(layer_kernel, n),
            out_shape=pltpu.VMEM((count, model), jnp.bfloat16),
            in_specs=[hbm] * 6,
            out_specs=vmem,
            scratch_shapes=[
                pltpu.VMEM((count, model), jnp.bfloat16),
                pltpu.VMEM((experts, model), jnp.bfloat16),
                pltpu.VMEM((2, count), jnp.int32),
                pltpu.VMEM((1, count), jnp.int32),
                pltpu.VMEM((model, hid), jnp.bfloat16),
                pltpu.VMEM((hid, model), jnp.bfloat16),
                buffer, buffer, buffer, buffer,
                pltpu.VMEM((CORES * capacity, hid), jnp.bfloat16),
                pltpu.VMEM((chips, count, CORES * capacity), jnp.bfloat16),
                pltpu.VMEM((count, model), jnp.float32),
                pltpu.VMEM((8, count), jnp.int32),
                pltpu.VMEM((2, CORES * capacity, count), jnp.bfloat16),
                pltpu.SemaphoreType.DMA((10,)),
                pltpu.SemaphoreType.DMA((chips, CORES)),
                pltpu.SemaphoreType.DMA((chips, CORES)),
                pltpu.SemaphoreType.DMA((chips, CORES)),
                pltpu.SemaphoreType.DMA((chips, CORES)),
            ],
            compiler_params=pltpu.CompilerParams(collective_id=0, has_side_effects=True, vmem_limit_bytes=50 * 2**20),
        )(*(pltpu.with_memory_space_constraint(x, pltpu.HBM) for x in (tokens[0], w_gate.T, expert_ids[0].T, keep_second, w_in[0], w_out[0])))
        return out[None]

    group_spec = P(("dp", "ep"))
    return jax.shard_map(local_layer, mesh=mesh, in_specs=(group_spec, P(), group_spec, group_spec, P("ep"), P("ep")), out_specs=group_spec, check_vma=False)
```

```python
import functools
import math

import jax
import jax.numpy as jnp
from jax import lax
from jax.experimental import pallas as pl
from jax.experimental.pallas import tpu as pltpu
from jax.sharding import PartitionSpec as P

MESH = pl.DeviceIdType.MESH
CORES = 2
LANES = 128


def route_slots(ids_ref, keep_ref, experts, capacity):
    tokens = ids_ref.shape[1]
    first = ids_ref[0:1, :]
    second = ids_ref[1:2, :]
    keep = keep_ref[0:1, :]
    expert_row = lax.broadcasted_iota(jnp.int32, (experts, tokens), 0)
    first_hot = jnp.where(expert_row == first, 1.0, 0.0)
    second_hot = jnp.where((expert_row == second) & (keep == 1), 1.0, 0.0)
    hot = jnp.concatenate([first_hot, second_hot], axis=0)
    blocks = tokens // LANES
    stacked = jnp.concatenate([hot[:, b * LANES:(b + 1) * LANES] for b in range(blocks)], axis=0).astype(jnp.bfloat16)
    row = lax.broadcasted_iota(jnp.int32, (LANES, 2 * LANES), 0)
    col = lax.broadcasted_iota(jnp.int32, (LANES, 2 * LANES), 1)
    before = jnp.where((row < col) | (col >= LANES), 1.0, 0.0).astype(jnp.bfloat16)
    counts = jnp.dot(stacked, before, preferred_element_type=jnp.float32)
    rows = 2 * experts
    offset = jnp.zeros((rows, LANES), jnp.float32)
    prefix = []
    for b in range(blocks):
        part = counts[b * rows:(b + 1) * rows]
        prefix.append(part[:, :LANES] + offset)
        offset = offset + part[:, LANES:]
    first_total = offset[:experts]
    slot_first, slot_second = [], []
    for b in range(blocks):
        lanes = slice(b * LANES, (b + 1) * LANES)
        pos_first = jnp.sum(prefix[b][:experts] * first_hot[:, lanes], axis=0, keepdims=True)
        pos_second = jnp.sum((prefix[b][experts:] + first_total) * second_hot[:, lanes], axis=0, keepdims=True)
        slot_first.append(pos_first)
        slot_second.append(pos_second)
    pos_first = jnp.concatenate(slot_first, axis=1).astype(jnp.int32)
    pos_second = jnp.concatenate(slot_second, axis=1).astype(jnp.int32)
    slot_first = jnp.where(pos_first < capacity, first * capacity + pos_first, -1)
    slot_second = jnp.where((keep == 1) & (pos_second < capacity), second * capacity + pos_second, -1)
    return slot_first, slot_second, first_hot, second_hot


def layer_kernel(n, groups, tokens_hbm, gate_hbm, ids_hbm, keep_hbm, w_in_hbm, w_out_hbm, out_ref,
                 tokens_ref, gate_ref, ids_ref, keep_ref, w_in, w_out, host_in, host_out, send, recv, back, ret, hidden, combine, total, slots,
                 load_sem, send_sem, recv_sem, back_sem, ret_sem, lend_sem, share_sem, slice_sem):
    me = lax.axis_index("ep")
    part = lax.axis_index("dp")
    chips = n // CORES
    half = chips // 2
    chip = me // CORES
    core = lax.rem(me, CORES)
    side = 1 - 2 * core
    experts = gate_ref.shape[0]
    tokens, model = tokens_ref.shape
    hid = w_in.shape[1]
    capacity = 2 * tokens // experts
    pair = CORES * capacity
    span = math.isqrt(groups)
    part_x = part // span
    part_y = lax.rem(part, span)

    load_ids = pltpu.make_async_copy(ids_hbm, ids_ref, load_sem.at[0])
    load_keep = pltpu.make_async_copy(keep_hbm, keep_ref, load_sem.at[1])
    load_gate = pltpu.make_async_copy(gate_hbm, gate_ref, load_sem.at[2])
    load_tokens = pltpu.make_async_copy(tokens_hbm, tokens_ref, load_sem.at[3])
    load_in = pltpu.make_async_copy(w_in_hbm, w_in, load_sem.at[4])
    load_out = pltpu.make_async_copy(w_out_hbm, w_out, load_sem.at[5])
    load_ids.start()
    load_keep.start()
    load_tokens.start()
    load_gate.start()

    def share_peer(array, phase, shift):
        if (array == 0) == (phase == 0):
            return lax.rem(part_x + shift, span) * span + part_y
        return part_x * span + lax.rem(part_y + shift, span)

    barrier = pltpu.get_barrier_semaphore()
    for k in range(1, n):
        pl.semaphore_signal(barrier, inc=1, device_id=(part, lax.rem(me + k, n)), device_id_type=MESH)
    for phase in range(2):
        for shift in range(1, span):
            pl.semaphore_signal(barrier, inc=1, device_id=(share_peer(0, phase, shift), me), device_id_type=MESH)

    load_ids.wait()
    load_keep.wait()
    slot_first, slot_second, first_hot, second_hot = route_slots(ids_ref, keep_ref, experts, capacity)
    slots[0:1, :] = slot_first
    slots[1:2, :] = slot_second

    def wrap(value):
        return lax.rem(value + chips, chips)

    def run_chip(hosted, j, c):
        sign = 1 - 2 * c
        return wrap(chip + sign * j) if hosted else wrap(chip - sign * j)

    def expert_of(hosted, j, c):
        sign = 1 - 2 * c
        return (wrap(run_chip(hosted, j, c) + sign) if hosted else run_chip(hosted, j, c)) * CORES + c

    def source_chip(hosted, j):
        return wrap(chip - side * j) if hosted else wrap(chip + side * j)

    def forward(hosted, j, c):
        step = hosted * half + j
        return pltpu.make_async_remote_copy(
            src_ref=send.at[step, c], dst_ref=recv.at[step, core],
            send_sem=send_sem.at[step, c], recv_sem=recv_sem.at[step, core],
            device_id=(part, run_chip(hosted, j, c) * CORES + c), device_id_type=MESH)

    def arrived(hosted, j, c):
        step = hosted * half + j
        return pltpu.make_async_remote_copy(
            src_ref=send.at[step, c], dst_ref=recv.at[step, c],
            send_sem=send_sem.at[step, c], recv_sem=recv_sem.at[step, c],
            device_id=(part, run_chip(hosted, j, c) * CORES + c), device_id_type=MESH)

    def reply(hosted, j, c):
        step = hosted * half + j
        return pltpu.make_async_remote_copy(
            src_ref=back.at[step, c], dst_ref=ret.at[step, core],
            send_sem=back_sem.at[step, c], recv_sem=ret_sem.at[step, core],
            device_id=(part, source_chip(hosted, j) * CORES + c), device_id_type=MESH)

    def returned(hosted, j, c):
        step = hosted * half + j
        return pltpu.make_async_remote_copy(
            src_ref=back.at[step, c], dst_ref=ret.at[step, c],
            send_sem=back_sem.at[step, c], recv_sem=ret_sem.at[step, c],
            device_id=(part, source_chip(hosted, j) * CORES + c), device_id_type=MESH)

    own_hbm = (w_in_hbm, w_out_hbm)
    host = (host_in, host_out)

    def slice_of(array, owner):
        rows = host[array].shape[0] // groups
        return pl.ds(pl.multiple_of(owner * rows, rows), rows)

    def lend(array):
        return pltpu.make_async_remote_copy(
            src_ref=own_hbm[array].at[slice_of(array, part)], dst_ref=host[array].at[slice_of(array, part)],
            send_sem=lend_sem.at[array], recv_sem=slice_sem.at[array, part],
            device_id=(part, wrap(chip - side) * CORES + core), device_id_type=MESH)

    def slice_owner(array, shift):
        return share_peer(array, 0, shift)

    def share(array, phase, k, shift):
        owner = slice_owner(array, k)
        return pltpu.make_async_remote_copy(
            src_ref=host[array].at[slice_of(array, owner)], dst_ref=host[array].at[slice_of(array, owner)],
            send_sem=share_sem.at[array, phase, k, shift], recv_sem=slice_sem.at[array, owner],
            device_id=(share_peer(array, phase, shift), me), device_id_type=MESH)

    def slice_ready(array, owner):
        return pltpu.make_async_remote_copy(
            src_ref=host[array].at[slice_of(array, owner)], dst_ref=host[array].at[slice_of(array, owner)],
            send_sem=lend_sem.at[array], recv_sem=slice_sem.at[array, owner],
            device_id=(share_peer(0, 0, 1), me), device_id_type=MESH)

    slot_row = lax.broadcasted_iota(jnp.int32, (capacity, tokens), 0)

    def pick_of(hosted, j):
        halves = []
        for c in range(CORES):
            base = expert_of(hosted, j, c) * capacity
            hit = (slot_row == slots[0:1, :] - base) | (slot_row == slots[1:2, :] - base)
            halves.append(jnp.where(hit, 1.0, 0.0))
        return jnp.concatenate(halves, axis=0).astype(jnp.bfloat16)

    def dispatch(hosted, j):
        rows = jnp.dot(pick_of(hosted, j), tokens_ref[...], preferred_element_type=jnp.float32).astype(jnp.bfloat16)
        send[hosted * half + j] = rows.reshape(CORES, capacity, model)

    load_tokens.wait()
    load_in.start()
    load_out.start()
    pl.semaphore_wait(barrier, n - 1 + 2 * (span - 1))
    lend(0).start()
    lend(1).start()
    far_first = range(half - 1, 0, -1)
    for hosted in range(2):
        for j in (*far_first, 0):
            dispatch(hosted, j)
    for hosted in range(2):
        forward(hosted, 0, 1 - core).start()
        recv[hosted * half, core] = send[hosted * half, core]

    load_gate.wait()
    logits = lax.dot_general(gate_ref[...], tokens_ref[...], (((1,), (1,)), ((), ())), preferred_element_type=jnp.float32)
    shifted = jnp.exp(logits - jnp.max(logits, axis=0, keepdims=True))
    probs = shifted / jnp.sum(shifted, axis=0, keepdims=True)
    gate_first = jnp.sum(probs * first_hot, axis=0, keepdims=True)
    gate_second = jnp.sum(probs * second_hot, axis=0, keepdims=True)
    gate_total = gate_first + gate_second
    gate_first = gate_first / gate_total
    gate_second = gate_second / gate_total
    for hosted in range(2):
        for j in range(half):
            weights = []
            for c in range(CORES):
                base = expert_of(hosted, j, c) * capacity
                weights.append(jnp.where(slot_row == slots[0:1, :] - base, gate_first, 0.0) + jnp.where(slot_row == slots[1:2, :] - base, gate_second, 0.0))
            combine[hosted * half + j] = jnp.concatenate(weights, axis=0).astype(jnp.bfloat16).T

    load_in.wait()
    load_out.wait()

    def experts_on(hosted, j):
        step = hosted * half + j
        up_ref, down_ref = (host_in, host_out) if hosted else (w_in, w_out)
        rows = recv[step].reshape(pair, model)
        tile = 512
        for t in range(hid // tile):
            cols = slice(t * tile, (t + 1) * tile)
            up = jnp.dot(rows, up_ref[:, cols], preferred_element_type=jnp.float32)
            hidden[:, cols] = jnp.maximum(up, 0.0).astype(jnp.bfloat16)
        tile = 256
        for t in range(model // tile):
            cols = slice(t * tile, (t + 1) * tile)
            down = jnp.dot(hidden[...], down_ref[:, cols], preferred_element_type=jnp.float32).astype(jnp.bfloat16)
            for c in range(CORES):
                back[step, c, :, cols] = down[c * capacity:(c + 1) * capacity]

    def local_experts(hosted):
        arrived(hosted, 0, 1 - core).wait_recv()
        experts_on(hosted, 0)
        reply(hosted, 0, 1 - core).start()
        ret[hosted * half, core] = back[hosted * half, core]

    def remote_experts(hosted):
        @pl.loop(0, half - 1)
        def _(index):
            j = half - 1 - index
            for c in range(CORES):
                arrived(hosted, j, c).wait_recv()
            experts_on(hosted, j)
            for c in (1, 0):
                reply(hosted, j, c).start()

    def first_share(array):
        slice_ready(array, part).wait_recv()
        for shift in range(1, span):
            share(array, 0, 0, shift).start()
        for shift in range(1, span):
            share(array, 1, 0, shift).start()

    def second_share(array):
        for k in range(1, span):
            slice_ready(array, slice_owner(array, k)).wait_recv()
            for shift in range(1, span):
                share(array, 1, k, shift).start()

    first_share(0)
    local_experts(0)
    for hosted in range(2):
        for j in far_first:
            for c in (core, 1 - core):
                forward(hosted, j, c).start()
    first_share(1)
    second_share(0)
    remote_experts(0)
    second_share(1)
    for array in range(2):
        for k in range(span):
            for shift in range(1, span):
                owner = share_peer(0, 0, k) // span * span + lax.rem(part_y + shift, span) if array == 0 else lax.rem(part_x + shift, span) * span + lax.rem(part_y + k, span)
                slice_ready(array, owner).wait_recv()
    local_experts(1)
    remote_experts(1)

    block = 256

    def mixed(step, r):
        return jnp.dot(combine[step, r * block:(r + 1) * block, :], ret[step].reshape(pair, model), preferred_element_type=jnp.float32)

    for hosted in range(2):
        returned(hosted, 0, 1 - core).wait_recv()
        for r in range(tokens // block):
            rows = slice(r * block, (r + 1) * block)
            if hosted == 0:
                total[rows, :] = mixed(0, r)
            else:
                total[rows, :] += mixed(half, r)
        count = half - 1 if hosted == 0 else half - 2

        @pl.loop(0, count)
        def _(index):
            j = half - 1 - index
            for c in range(CORES):
                returned(hosted, j, c).wait_recv()
            for r in range(tokens // block):
                total[r * block:(r + 1) * block, :] += mixed(hosted * half + j, r)

    for c in range(CORES):
        returned(1, 1, c).wait_recv()
    for r in range(tokens // block):
        rows = slice(r * block, (r + 1) * block)
        out_ref[rows, :] = (total[rows, :] + mixed(half + 1, r)).astype(jnp.bfloat16)

    for hosted in range(2):
        forward(hosted, 0, 1 - core).wait_send()
        reply(hosted, 0, 1 - core).wait_send()

        @pl.loop(1, half)
        def _(j):
            for c in range(CORES):
                forward(hosted, j, c).wait_send()
                reply(hosted, j, c).wait_send()
    for array in range(2):
        lend(array).wait_send()
        for phase in range(2):
            for k in range(span if phase == 1 else 1):
                for shift in range(1, span):
                    share(array, phase, k, shift).wait_send()


def solution(mesh):
    n = mesh.shape["ep"]
    chips = n // CORES
    groups = mesh.shape["dp"]
    span = math.isqrt(groups)

    def local_layer(tokens, w_gate, expert_ids, keep_second, w_in, w_out):
        count, model = tokens.shape[1:]
        experts = w_gate.shape[1]
        hid = w_in.shape[2]
        capacity = 2 * count // experts
        buffer = pltpu.VMEM((chips, CORES, capacity, model), jnp.bfloat16)
        vmem = pl.BlockSpec(memory_space=pltpu.VMEM)
        hbm = pl.BlockSpec(memory_space=pltpu.HBM)
        out = pl.pallas_call(
            functools.partial(layer_kernel, n, groups),
            out_shape=pltpu.VMEM((count, model), jnp.bfloat16),
            in_specs=[hbm] * 6,
            out_specs=vmem,
            scratch_shapes=[
                pltpu.VMEM((count, model), jnp.bfloat16),
                pltpu.VMEM((experts, model), jnp.bfloat16),
                pltpu.VMEM((2, count), jnp.int32),
                pltpu.VMEM((1, count), jnp.int32),
                pltpu.VMEM((model, hid), jnp.bfloat16),
                pltpu.VMEM((hid, model), jnp.bfloat16),
                pltpu.VMEM((model, hid), jnp.bfloat16),
                pltpu.VMEM((hid, model), jnp.bfloat16),
                buffer, buffer, buffer, buffer,
                pltpu.VMEM((CORES * capacity, hid), jnp.bfloat16),
                pltpu.VMEM((chips, count, CORES * capacity), jnp.bfloat16),
                pltpu.VMEM((count, model), jnp.float32),
                pltpu.VMEM((8, count), jnp.int32),
                pltpu.SemaphoreType.DMA((6,)),
                pltpu.SemaphoreType.DMA((chips, CORES)),
                pltpu.SemaphoreType.DMA((chips, CORES)),
                pltpu.SemaphoreType.DMA((chips, CORES)),
                pltpu.SemaphoreType.DMA((chips, CORES)),
                pltpu.SemaphoreType.DMA((2,)),
                pltpu.SemaphoreType.DMA((2, 2, span, span)),
                pltpu.SemaphoreType.DMA((2, groups)),
            ],
            compiler_params=pltpu.CompilerParams(collective_id=0, has_side_effects=True, vmem_limit_bytes=54 * 2**20),
        )(*(pltpu.with_memory_space_constraint(x, pltpu.HBM) for x in (tokens[0], w_gate.T, expert_ids[0].T, keep_second, w_in[0], w_out[0])))
        return out[None]

    group_spec = P(("dp", "ep"))
    return jax.shard_map(local_layer, mesh=mesh, in_specs=(group_spec, P(), group_spec, group_spec, P("ep"), P("ep")), out_specs=group_spec, check_vma=False)
```

```python
import functools
import math

import jax
import jax.numpy as jnp
from jax import lax
from jax.experimental import pallas as pl
from jax.experimental.pallas import tpu as pltpu
from jax.sharding import PartitionSpec as P

MESH = pl.DeviceIdType.MESH
CORES = 2
LANES = 128


def route_slots(ids_ref, keep_ref, experts, capacity):
    tokens = ids_ref.shape[1]
    first = ids_ref[0:1, :]
    second = ids_ref[1:2, :]
    keep = keep_ref[0:1, :]
    expert_row = lax.broadcasted_iota(jnp.int32, (experts, tokens), 0)
    first_hot = jnp.where(expert_row == first, 1.0, 0.0)
    second_hot = jnp.where((expert_row == second) & (keep == 1), 1.0, 0.0)
    hot = jnp.concatenate([first_hot, second_hot], axis=0)
    blocks = tokens // LANES
    stacked = jnp.concatenate([hot[:, b * LANES:(b + 1) * LANES] for b in range(blocks)], axis=0).astype(jnp.bfloat16)
    row = lax.broadcasted_iota(jnp.int32, (LANES, 2 * LANES), 0)
    col = lax.broadcasted_iota(jnp.int32, (LANES, 2 * LANES), 1)
    before = jnp.where((row < col) | (col >= LANES), 1.0, 0.0).astype(jnp.bfloat16)
    counts = jnp.dot(stacked, before, preferred_element_type=jnp.float32)
    rows = 2 * experts
    offset = jnp.zeros((rows, LANES), jnp.float32)
    prefix = []
    for b in range(blocks):
        part = counts[b * rows:(b + 1) * rows]
        prefix.append(part[:, :LANES] + offset)
        offset = offset + part[:, LANES:]
    first_total = offset[:experts]
    slot_first, slot_second = [], []
    for b in range(blocks):
        lanes = slice(b * LANES, (b + 1) * LANES)
        pos_first = jnp.sum(prefix[b][:experts] * first_hot[:, lanes], axis=0, keepdims=True)
        pos_second = jnp.sum((prefix[b][experts:] + first_total) * second_hot[:, lanes], axis=0, keepdims=True)
        slot_first.append(pos_first)
        slot_second.append(pos_second)
    pos_first = jnp.concatenate(slot_first, axis=1).astype(jnp.int32)
    pos_second = jnp.concatenate(slot_second, axis=1).astype(jnp.int32)
    slot_first = jnp.where(pos_first < capacity, first * capacity + pos_first, -1)
    slot_second = jnp.where((keep == 1) & (pos_second < capacity), second * capacity + pos_second, -1)
    return slot_first, slot_second, first_hot, second_hot


def layer_kernel(n, groups, tokens_hbm, gate_hbm, ids_hbm, keep_hbm, w_in_hbm, w_out_hbm, out_ref,
                 tokens_ref, gate_ref, ids_ref, keep_ref, w_in, w_out, host_in, host_out, send, recv, back, ret, hidden, combine, total, slots,
                 load_sem, send_sem, recv_sem, back_sem, ret_sem, lend_sem, share_sem, slice_sem, reach_sem):
    me = lax.axis_index("ep")
    part = lax.axis_index("dp")
    chips = n // CORES
    half = chips // 2
    chip = me // CORES
    core = lax.rem(me, CORES)
    side = 1 - 2 * core
    experts = gate_ref.shape[0]
    tokens, model = tokens_ref.shape
    hid = w_in.shape[1]
    capacity = 2 * tokens // experts
    pair = CORES * capacity
    span = math.isqrt(groups)
    part_x = part // span
    part_y = lax.rem(part, span)

    load_ids = pltpu.make_async_copy(ids_hbm, ids_ref, load_sem.at[0])
    load_keep = pltpu.make_async_copy(keep_hbm, keep_ref, load_sem.at[1])
    load_gate = pltpu.make_async_copy(gate_hbm, gate_ref, load_sem.at[2])
    load_tokens = pltpu.make_async_copy(tokens_hbm, tokens_ref, load_sem.at[3])
    load_in = pltpu.make_async_copy(w_in_hbm, w_in, load_sem.at[4])
    load_out = pltpu.make_async_copy(w_out_hbm, w_out, load_sem.at[5])
    load_ids.start()
    load_keep.start()
    load_tokens.start()
    load_gate.start()

    def share_peer(array, phase, shift):
        if (array == 0) == (phase == 0):
            return lax.rem(part_x + shift, span) * span + part_y
        return part_x * span + lax.rem(part_y + shift, span)

    barrier = pltpu.get_barrier_semaphore()
    ahead, behind, partner = lax.rem(me + CORES, n), lax.rem(me + n - CORES, n), me + 1 - 2 * core
    for near in (ahead, behind, partner):
        pl.semaphore_signal(barrier, inc=1, device_id=(part, near), device_id_type=MESH)
    for phase in range(2):
        for shift in range(1, span):
            pl.semaphore_signal(barrier, inc=1, device_id=(share_peer(0, phase, shift), me), device_id_type=MESH)


    def wrap(value):
        return lax.rem(value + chips, chips)

    def run_chip(hosted, j, c):
        sign = 1 - 2 * c
        return wrap(chip + sign * j) if hosted else wrap(chip - sign * j)

    def expert_of(hosted, j, c):
        sign = 1 - 2 * c
        return (wrap(run_chip(hosted, j, c) + sign) if hosted else run_chip(hosted, j, c)) * CORES + c

    def source_chip(hosted, j):
        return wrap(chip - side * j) if hosted else wrap(chip + side * j)

    def forward(hosted, j, c):
        step = hosted * half + j
        return pltpu.make_async_remote_copy(
            src_ref=send.at[step, c], dst_ref=recv.at[step, core],
            send_sem=send_sem.at[step, c], recv_sem=recv_sem.at[step, core],
            device_id=(part, run_chip(hosted, j, c) * CORES + c), device_id_type=MESH)

    def arrived(hosted, j, c):
        step = hosted * half + j
        return pltpu.make_async_remote_copy(
            src_ref=send.at[step, c], dst_ref=recv.at[step, c],
            send_sem=send_sem.at[step, c], recv_sem=recv_sem.at[step, c],
            device_id=(part, run_chip(hosted, j, c) * CORES + c), device_id_type=MESH)

    def reply(hosted, j, c):
        step = hosted * half + j
        return pltpu.make_async_remote_copy(
            src_ref=back.at[step, c], dst_ref=ret.at[step, core],
            send_sem=back_sem.at[step, c], recv_sem=ret_sem.at[step, core],
            device_id=(part, source_chip(hosted, j) * CORES + c), device_id_type=MESH)

    def returned(hosted, j, c):
        step = hosted * half + j
        return pltpu.make_async_remote_copy(
            src_ref=back.at[step, c], dst_ref=ret.at[step, c],
            send_sem=back_sem.at[step, c], recv_sem=ret_sem.at[step, c],
            device_id=(part, source_chip(hosted, j) * CORES + c), device_id_type=MESH)

    own_hbm = (w_in_hbm, w_out_hbm)
    host = (host_in, host_out)

    def slice_of(array, owner):
        rows = host[array].shape[0] // groups
        return pl.ds(pl.multiple_of(owner * rows, rows), rows)

    def lend(array):
        return pltpu.make_async_remote_copy(
            src_ref=own_hbm[array].at[slice_of(array, part)], dst_ref=host[array].at[slice_of(array, part)],
            send_sem=lend_sem.at[array], recv_sem=slice_sem.at[array, part],
            device_id=(part, wrap(chip - side) * CORES + core), device_id_type=MESH)

    pl.semaphore_wait(barrier, 3 + 2 * (span - 1))
    lend(0).start()
    lend(1).start()
    for level in range(half - 1):
        for near in (ahead, behind):
            pl.semaphore_signal(reach_sem.at[level], inc=1, device_id=(part, near), device_id_type=MESH)
        pl.semaphore_wait(reach_sem.at[level], 2)
    pl.semaphore_signal(reach_sem.at[half - 1], inc=1, device_id=(part, partner), device_id_type=MESH)
    pl.semaphore_wait(reach_sem.at[half - 1], 1)

    load_ids.wait()
    load_keep.wait()
    slot_first, slot_second, first_hot, second_hot = route_slots(ids_ref, keep_ref, experts, capacity)
    slots[0:1, :] = slot_first
    slots[1:2, :] = slot_second

    def slice_owner(array, shift):
        return share_peer(array, 0, shift)

    def share(array, phase, k, shift):
        owner = slice_owner(array, k)
        return pltpu.make_async_remote_copy(
            src_ref=host[array].at[slice_of(array, owner)], dst_ref=host[array].at[slice_of(array, owner)],
            send_sem=share_sem.at[array, phase, k, shift], recv_sem=slice_sem.at[array, owner],
            device_id=(share_peer(array, phase, shift), me), device_id_type=MESH)

    def slice_ready(array, owner):
        return pltpu.make_async_remote_copy(
            src_ref=host[array].at[slice_of(array, owner)], dst_ref=host[array].at[slice_of(array, owner)],
            send_sem=lend_sem.at[array], recv_sem=slice_sem.at[array, owner],
            device_id=(share_peer(0, 0, 1), me), device_id_type=MESH)

    slot_row = lax.broadcasted_iota(jnp.int32, (capacity, tokens), 0)

    def pick_of(hosted, j):
        halves = []
        for c in range(CORES):
            base = expert_of(hosted, j, c) * capacity
            hit = (slot_row == slots[0:1, :] - base) | (slot_row == slots[1:2, :] - base)
            halves.append(jnp.where(hit, 1.0, 0.0))
        return jnp.concatenate(halves, axis=0).astype(jnp.bfloat16)

    def dispatch(hosted, j):
        rows = jnp.dot(pick_of(hosted, j), tokens_ref[...], preferred_element_type=jnp.float32).astype(jnp.bfloat16)
        send[hosted * half + j] = rows.reshape(CORES, capacity, model)

    load_tokens.wait()
    load_in.start()
    load_out.start()
    far_first = range(half - 1, 0, -1)
    for hosted in range(2):
        for j in (*far_first, 0):
            dispatch(hosted, j)
    for hosted in range(2):
        forward(hosted, 0, 1 - core).start()
        recv[hosted * half, core] = send[hosted * half, core]

    load_gate.wait()
    logits = lax.dot_general(gate_ref[...], tokens_ref[...], (((1,), (1,)), ((), ())), preferred_element_type=jnp.float32)
    shifted = jnp.exp(logits - jnp.max(logits, axis=0, keepdims=True))
    probs = shifted / jnp.sum(shifted, axis=0, keepdims=True)
    gate_first = jnp.sum(probs * first_hot, axis=0, keepdims=True)
    gate_second = jnp.sum(probs * second_hot, axis=0, keepdims=True)
    gate_total = gate_first + gate_second
    gate_first = gate_first / gate_total
    gate_second = gate_second / gate_total
    for hosted in range(2):
        for j in range(half):
            weights = []
            for c in range(CORES):
                base = expert_of(hosted, j, c) * capacity
                weights.append(jnp.where(slot_row == slots[0:1, :] - base, gate_first, 0.0) + jnp.where(slot_row == slots[1:2, :] - base, gate_second, 0.0))
            combine[hosted * half + j] = jnp.concatenate(weights, axis=0).astype(jnp.bfloat16).T

    load_in.wait()
    load_out.wait()

    def experts_on(hosted, j):
        step = hosted * half + j
        up_ref, down_ref = (host_in, host_out) if hosted else (w_in, w_out)
        rows = recv[step].reshape(pair, model)
        tile = 512
        for t in range(hid // tile):
            cols = slice(t * tile, (t + 1) * tile)
            up = jnp.dot(rows, up_ref[:, cols], preferred_element_type=jnp.float32)
            hidden[:, cols] = jnp.maximum(up, 0.0).astype(jnp.bfloat16)
        tile = 256
        for t in range(model // tile):
            cols = slice(t * tile, (t + 1) * tile)
            down = jnp.dot(hidden[...], down_ref[:, cols], preferred_element_type=jnp.float32).astype(jnp.bfloat16)
            for c in range(CORES):
                back[step, c, :, cols] = down[c * capacity:(c + 1) * capacity]

    def local_experts(hosted):
        arrived(hosted, 0, 1 - core).wait_recv()
        experts_on(hosted, 0)
        reply(hosted, 0, 1 - core).start()
        ret[hosted * half, core] = back[hosted * half, core]

    def remote_experts(hosted):
        @pl.loop(0, half - 1)
        def _(index):
            j = half - 1 - index
            for c in range(CORES):
                arrived(hosted, j, c).wait_recv()
            experts_on(hosted, j)
            for c in (1, 0):
                reply(hosted, j, c).start()

    def first_share(array):
        slice_ready(array, part).wait_recv()
        for shift in range(1, span):
            share(array, 0, 0, shift).start()
        for shift in range(1, span):
            share(array, 1, 0, shift).start()

    def second_share(array):
        for k in range(1, span):
            slice_ready(array, slice_owner(array, k)).wait_recv()
            for shift in range(1, span):
                share(array, 1, k, shift).start()

    first_share(0)
    local_experts(0)
    for hosted in range(2):
        for j in far_first:
            for c in (core, 1 - core):
                forward(hosted, j, c).start()
    first_share(1)
    second_share(0)
    remote_experts(0)
    second_share(1)
    for array in range(2):
        for k in range(span):
            for shift in range(1, span):
                owner = share_peer(0, 0, k) // span * span + lax.rem(part_y + shift, span) if array == 0 else lax.rem(part_x + shift, span) * span + lax.rem(part_y + k, span)
                slice_ready(array, owner).wait_recv()
    remote_experts(1)
    local_experts(1)

    block = 256

    def mixed(step, r):
        return jnp.dot(combine[step, r * block:(r + 1) * block, :], ret[step].reshape(pair, model), preferred_element_type=jnp.float32)

    for hosted in range(2):
        returned(hosted, 0, 1 - core).wait_recv()
        for r in range(tokens // block):
            rows = slice(r * block, (r + 1) * block)
            if hosted == 0:
                total[rows, :] = mixed(0, r)
            else:
                total[rows, :] += mixed(half, r)
        count = half - 1 if hosted == 0 else half - 2

        @pl.loop(0, count)
        def _(index):
            j = half - 1 - index
            for c in range(CORES):
                returned(hosted, j, c).wait_recv()
            for r in range(tokens // block):
                total[r * block:(r + 1) * block, :] += mixed(hosted * half + j, r)

    for c in range(CORES):
        returned(1, 1, c).wait_recv()
    for r in range(tokens // block):
        rows = slice(r * block, (r + 1) * block)
        out_ref[rows, :] = (total[rows, :] + mixed(half + 1, r)).astype(jnp.bfloat16)

    for hosted in range(2):
        forward(hosted, 0, 1 - core).wait_send()
        reply(hosted, 0, 1 - core).wait_send()

        @pl.loop(1, half)
        def _(j):
            for c in range(CORES):
                forward(hosted, j, c).wait_send()
                reply(hosted, j, c).wait_send()
    for array in range(2):
        lend(array).wait_send()
        for phase in range(2):
            for k in range(span if phase == 1 else 1):
                for shift in range(1, span):
                    share(array, phase, k, shift).wait_send()


def solution(mesh):
    n = mesh.shape["ep"]
    chips = n // CORES
    groups = mesh.shape["dp"]
    span = math.isqrt(groups)

    def local_layer(tokens, w_gate, expert_ids, keep_second, w_in, w_out):
        count, model = tokens.shape[1:]
        experts = w_gate.shape[1]
        hid = w_in.shape[2]
        capacity = 2 * count // experts
        buffer = pltpu.VMEM((chips, CORES, capacity, model), jnp.bfloat16)
        vmem = pl.BlockSpec(memory_space=pltpu.VMEM)
        hbm = pl.BlockSpec(memory_space=pltpu.HBM)
        out = pl.pallas_call(
            functools.partial(layer_kernel, n, groups),
            out_shape=pltpu.VMEM((count, model), jnp.bfloat16),
            in_specs=[hbm] * 6,
            out_specs=vmem,
            scratch_shapes=[
                pltpu.VMEM((count, model), jnp.bfloat16),
                pltpu.VMEM((experts, model), jnp.bfloat16),
                pltpu.VMEM((2, count), jnp.int32),
                pltpu.VMEM((1, count), jnp.int32),
                pltpu.VMEM((model, hid), jnp.bfloat16),
                pltpu.VMEM((hid, model), jnp.bfloat16),
                pltpu.VMEM((model, hid), jnp.bfloat16),
                pltpu.VMEM((hid, model), jnp.bfloat16),
                buffer, buffer, buffer, buffer,
                pltpu.VMEM((CORES * capacity, hid), jnp.bfloat16),
                pltpu.VMEM((chips, count, CORES * capacity), jnp.bfloat16),
                pltpu.VMEM((count, model), jnp.float32),
                pltpu.VMEM((8, count), jnp.int32),
                pltpu.SemaphoreType.DMA((6,)),
                pltpu.SemaphoreType.DMA((chips, CORES)),
                pltpu.SemaphoreType.DMA((chips, CORES)),
                pltpu.SemaphoreType.DMA((chips, CORES)),
                pltpu.SemaphoreType.DMA((chips, CORES)),
                pltpu.SemaphoreType.DMA((2,)),
                pltpu.SemaphoreType.DMA((2, 2, span, span)),
                pltpu.SemaphoreType.DMA((2, groups)),
                pltpu.SemaphoreType.REGULAR((chips // 2,)),
            ],
            compiler_params=pltpu.CompilerParams(collective_id=0, has_side_effects=True, vmem_limit_bytes=54 * 2**20),
        )(*(pltpu.with_memory_space_constraint(x, pltpu.HBM) for x in (tokens[0], w_gate.T, expert_ids[0].T, keep_second, w_in[0], w_out[0])))
        return out[None]

    group_spec = P(("dp", "ep"))
    return jax.shard_map(local_layer, mesh=mesh, in_specs=(group_spec, P(), group_spec, group_spec, P("ep"), P("ep")), out_specs=group_spec, check_vma=False)
```

```python
import functools
import math

import jax
import jax.numpy as jnp
from jax import lax
from jax.experimental import pallas as pl
from jax.experimental.pallas import tpu as pltpu
from jax.sharding import PartitionSpec as P

MESH = pl.DeviceIdType.MESH
CORES = 2
LANES = 128


def route_slots(ids_ref, keep_ref, experts, capacity):
    tokens = ids_ref.shape[1]
    first = ids_ref[0:1, :]
    second = ids_ref[1:2, :]
    keep = keep_ref[0:1, :]
    expert_row = lax.broadcasted_iota(jnp.int32, (experts, tokens), 0)
    first_hot = jnp.where(expert_row == first, 1.0, 0.0)
    second_hot = jnp.where((expert_row == second) & (keep == 1), 1.0, 0.0)
    hot = jnp.concatenate([first_hot, second_hot], axis=0)
    blocks = tokens // LANES
    stacked = jnp.concatenate([hot[:, b * LANES:(b + 1) * LANES] for b in range(blocks)], axis=0).astype(jnp.bfloat16)
    row = lax.broadcasted_iota(jnp.int32, (LANES, 2 * LANES), 0)
    col = lax.broadcasted_iota(jnp.int32, (LANES, 2 * LANES), 1)
    before = jnp.where((row < col) | (col >= LANES), 1.0, 0.0).astype(jnp.bfloat16)
    counts = jnp.dot(stacked, before, preferred_element_type=jnp.float32)
    rows = 2 * experts
    offset = jnp.zeros((rows, LANES), jnp.float32)
    prefix = []
    for b in range(blocks):
        part = counts[b * rows:(b + 1) * rows]
        prefix.append(part[:, :LANES] + offset)
        offset = offset + part[:, LANES:]
    first_total = offset[:experts]
    slot_first, slot_second = [], []
    for b in range(blocks):
        lanes = slice(b * LANES, (b + 1) * LANES)
        pos_first = jnp.sum(prefix[b][:experts] * first_hot[:, lanes], axis=0, keepdims=True)
        pos_second = jnp.sum((prefix[b][experts:] + first_total) * second_hot[:, lanes], axis=0, keepdims=True)
        slot_first.append(pos_first)
        slot_second.append(pos_second)
    pos_first = jnp.concatenate(slot_first, axis=1).astype(jnp.int32)
    pos_second = jnp.concatenate(slot_second, axis=1).astype(jnp.int32)
    slot_first = jnp.where(pos_first < capacity, first * capacity + pos_first, -1)
    slot_second = jnp.where((keep == 1) & (pos_second < capacity), second * capacity + pos_second, -1)
    return slot_first, slot_second, first_hot, second_hot


def layer_kernel(n, groups, tokens_hbm, gate_hbm, ids_hbm, keep_hbm, w_in_hbm, w_out_hbm, out_ref,
                 tokens_ref, gate_ref, ids_ref, keep_ref, w_in, w_out, host_in, host_out, send, recv, back, ret, hidden, combine, total, slots,
                 load_sem, send_sem, recv_sem, back_sem, ret_sem, lend_sem, share_sem, slice_sem, reach_sem):
    me = lax.axis_index("ep")
    part = lax.axis_index("dp")
    chips = n // CORES
    half = chips // 2
    chip = me // CORES
    core = lax.rem(me, CORES)
    side = 1 - 2 * core
    experts = gate_ref.shape[0]
    tokens, model = tokens_ref.shape
    hid = w_in.shape[1]
    capacity = 2 * tokens // experts
    pair = CORES * capacity
    span = math.isqrt(groups)
    part_x = part // span
    part_y = lax.rem(part, span)

    load_ids = pltpu.make_async_copy(ids_hbm, ids_ref, load_sem.at[0])
    load_keep = pltpu.make_async_copy(keep_hbm, keep_ref, load_sem.at[1])
    load_gate = pltpu.make_async_copy(gate_hbm, gate_ref, load_sem.at[2])
    load_tokens = pltpu.make_async_copy(tokens_hbm, tokens_ref, load_sem.at[3])
    load_in = pltpu.make_async_copy(w_in_hbm, w_in, load_sem.at[4])
    load_out = pltpu.make_async_copy(w_out_hbm, w_out, load_sem.at[5])
    load_ids.start()
    load_keep.start()
    load_tokens.start()
    load_gate.start()

    def share_peer(array, phase, shift):
        if (array == 0) == (phase == 0):
            return lax.rem(part_x + shift, span) * span + part_y
        return part_x * span + lax.rem(part_y + shift, span)

    barrier = pltpu.get_barrier_semaphore()
    ahead, behind, partner = lax.rem(me + CORES, n), lax.rem(me + n - CORES, n), me + 1 - 2 * core
    for near in (ahead, behind, partner):
        pl.semaphore_signal(barrier, inc=1, device_id=(part, near), device_id_type=MESH)
    for phase in range(2):
        for shift in range(1, span):
            pl.semaphore_signal(barrier, inc=1, device_id=(share_peer(0, phase, shift), me), device_id_type=MESH)


    def wrap(value):
        return lax.rem(value + chips, chips)

    def run_chip(hosted, j, c):
        sign = 1 - 2 * c
        return wrap(chip + sign * j) if hosted else wrap(chip - sign * j)

    def expert_of(hosted, j, c):
        sign = 1 - 2 * c
        return (wrap(run_chip(hosted, j, c) + sign) if hosted else run_chip(hosted, j, c)) * CORES + c

    def source_chip(hosted, j):
        return wrap(chip - side * j) if hosted else wrap(chip + side * j)

    def forward(hosted, j, c):
        step = hosted * half + j
        return pltpu.make_async_remote_copy(
            src_ref=send.at[step, c], dst_ref=recv.at[step, core],
            send_sem=send_sem.at[step, c], recv_sem=recv_sem.at[step, core],
            device_id=(part, run_chip(hosted, j, c) * CORES + c), device_id_type=MESH)

    def arrived(hosted, j, c):
        step = hosted * half + j
        return pltpu.make_async_remote_copy(
            src_ref=send.at[step, c], dst_ref=recv.at[step, c],
            send_sem=send_sem.at[step, c], recv_sem=recv_sem.at[step, c],
            device_id=(part, run_chip(hosted, j, c) * CORES + c), device_id_type=MESH)

    def reply(hosted, j, c):
        step = hosted * half + j
        return pltpu.make_async_remote_copy(
            src_ref=back.at[step, c], dst_ref=ret.at[step, core],
            send_sem=back_sem.at[step, c], recv_sem=ret_sem.at[step, core],
            device_id=(part, source_chip(hosted, j) * CORES + c), device_id_type=MESH)

    def returned(hosted, j, c):
        step = hosted * half + j
        return pltpu.make_async_remote_copy(
            src_ref=back.at[step, c], dst_ref=ret.at[step, c],
            send_sem=back_sem.at[step, c], recv_sem=ret_sem.at[step, c],
            device_id=(part, source_chip(hosted, j) * CORES + c), device_id_type=MESH)

    own_hbm = (w_in_hbm, w_out_hbm)
    host = (host_in, host_out)

    def slice_of(array, owner):
        rows = host[array].shape[0] // groups
        return pl.ds(pl.multiple_of(owner * rows, rows), rows)

    def lend(array):
        return pltpu.make_async_remote_copy(
            src_ref=own_hbm[array].at[slice_of(array, part)], dst_ref=host[array].at[slice_of(array, part)],
            send_sem=lend_sem.at[array], recv_sem=slice_sem.at[array, part],
            device_id=(part, wrap(chip - side) * CORES + core), device_id_type=MESH)

    pl.semaphore_wait(barrier, 3 + 2 * (span - 1))
    lend(0).start()
    lend(1).start()
    for level in range(half - 1):
        for near in (ahead, behind):
            pl.semaphore_signal(reach_sem.at[level], inc=1, device_id=(part, near), device_id_type=MESH)
        pl.semaphore_wait(reach_sem.at[level], 2)
    pl.semaphore_signal(reach_sem.at[half - 1], inc=1, device_id=(part, partner), device_id_type=MESH)
    pl.semaphore_wait(reach_sem.at[half - 1], 1)

    load_ids.wait()
    load_keep.wait()
    slot_first, slot_second, first_hot, second_hot = route_slots(ids_ref, keep_ref, experts, capacity)
    slots[0:1, :] = slot_first
    slots[1:2, :] = slot_second

    def slice_owner(array, shift):
        return share_peer(array, 0, shift)

    def share(array, phase, k, shift):
        owner = slice_owner(array, k)
        return pltpu.make_async_remote_copy(
            src_ref=host[array].at[slice_of(array, owner)], dst_ref=host[array].at[slice_of(array, owner)],
            send_sem=share_sem.at[array, phase, k, shift], recv_sem=slice_sem.at[array, owner],
            device_id=(share_peer(array, phase, shift), me), device_id_type=MESH)

    def slice_ready(array, owner):
        return pltpu.make_async_remote_copy(
            src_ref=host[array].at[slice_of(array, owner)], dst_ref=host[array].at[slice_of(array, owner)],
            send_sem=lend_sem.at[array], recv_sem=slice_sem.at[array, owner],
            device_id=(share_peer(0, 0, 1), me), device_id_type=MESH)

    slot_row = lax.broadcasted_iota(jnp.int32, (capacity, tokens), 0)

    def pick_of(hosted, j):
        halves = []
        for c in range(CORES):
            base = expert_of(hosted, j, c) * capacity
            hit = (slot_row == slots[0:1, :] - base) | (slot_row == slots[1:2, :] - base)
            halves.append(jnp.where(hit, 1.0, 0.0))
        return jnp.concatenate(halves, axis=0).astype(jnp.bfloat16)

    def dispatch(hosted, j):
        rows = jnp.dot(pick_of(hosted, j), tokens_ref[...], preferred_element_type=jnp.float32).astype(jnp.bfloat16)
        send[hosted * half + j] = rows.reshape(CORES, capacity, model)

    load_tokens.wait()
    load_in.start()
    load_out.start()
    far_first = range(half - 1, 0, -1)
    for hosted in range(2):
        for j in (*far_first, 0):
            dispatch(hosted, j)
    for hosted in range(2):
        forward(hosted, 0, 1 - core).start()
        recv[hosted * half, core] = send[hosted * half, core]

    load_gate.wait()
    logits = lax.dot_general(gate_ref[...], tokens_ref[...], (((1,), (1,)), ((), ())), preferred_element_type=jnp.float32)
    shifted = jnp.exp(logits - jnp.max(logits, axis=0, keepdims=True))
    probs = shifted / jnp.sum(shifted, axis=0, keepdims=True)
    gate_first = jnp.sum(probs * first_hot, axis=0, keepdims=True)
    gate_second = jnp.sum(probs * second_hot, axis=0, keepdims=True)
    gate_total = gate_first + gate_second
    gate_first = gate_first / gate_total
    gate_second = gate_second / gate_total
    for hosted in range(2):
        for j in range(half):
            weights = []
            for c in range(CORES):
                base = expert_of(hosted, j, c) * capacity
                weights.append(jnp.where(slot_row == slots[0:1, :] - base, gate_first, 0.0) + jnp.where(slot_row == slots[1:2, :] - base, gate_second, 0.0))
            combine[hosted * half + j] = jnp.concatenate(weights, axis=0).astype(jnp.bfloat16).T

    load_in.wait()
    load_out.wait()

    def experts_on(hosted, j):
        step = hosted * half + j
        up_ref, down_ref = (host_in, host_out) if hosted else (w_in, w_out)
        rows = recv[step].reshape(pair, model)
        tile = 512
        for t in range(hid // tile):
            cols = slice(t * tile, (t + 1) * tile)
            up = jnp.dot(rows, up_ref[:, cols], preferred_element_type=jnp.float32)
            hidden[:, cols] = jnp.maximum(up, 0.0).astype(jnp.bfloat16)
        tile = 256
        for t in range(model // tile):
            cols = slice(t * tile, (t + 1) * tile)
            down = jnp.dot(hidden[...], down_ref[:, cols], preferred_element_type=jnp.float32).astype(jnp.bfloat16)
            for c in range(CORES):
                back[step, c, :, cols] = down[c * capacity:(c + 1) * capacity]

    def local_experts(hosted):
        arrived(hosted, 0, 1 - core).wait_recv()
        experts_on(hosted, 0)
        reply(hosted, 0, 1 - core).start()
        ret[hosted * half, core] = back[hosted * half, core]

    def remote_experts(hosted):
        @pl.loop(0, half - 1)
        def _(index):
            j = half - 1 - index
            for c in range(CORES):
                arrived(hosted, j, c).wait_recv()
            experts_on(hosted, j)
            for c in (1, 0):
                reply(hosted, j, c).start()

    def first_share(array):
        slice_ready(array, part).wait_recv()
        for shift in range(1, span):
            share(array, 0, 0, shift).start()
        for shift in range(1, span):
            share(array, 1, 0, shift).start()

    def second_share(array):
        for k in range(1, span):
            slice_ready(array, slice_owner(array, k)).wait_recv()
            for shift in range(1, span):
                share(array, 1, k, shift).start()

    first_share(0)
    local_experts(0)
    for hosted in range(1):
        for j in far_first:
            for c in (core, 1 - core):
                forward(hosted, j, c).start()
    first_share(1)
    for hosted in range(1, 2):
        for j in far_first:
            for c in (core, 1 - core):
                forward(hosted, j, c).start()
    second_share(0)
    remote_experts(0)
    second_share(1)
    for array in range(2):
        for k in range(span):
            for shift in range(1, span):
                owner = share_peer(0, 0, k) // span * span + lax.rem(part_y + shift, span) if array == 0 else lax.rem(part_x + shift, span) * span + lax.rem(part_y + k, span)
                slice_ready(array, owner).wait_recv()
    remote_experts(1)
    local_experts(1)

    block = 256

    def mixed(step, r):
        return jnp.dot(combine[step, r * block:(r + 1) * block, :], ret[step].reshape(pair, model), preferred_element_type=jnp.float32)

    for hosted in range(2):
        returned(hosted, 0, 1 - core).wait_recv()
        for r in range(tokens // block):
            rows = slice(r * block, (r + 1) * block)
            if hosted == 0:
                total[rows, :] = mixed(0, r)
            else:
                total[rows, :] += mixed(half, r)
        count = half - 1 if hosted == 0 else half - 2

        @pl.loop(0, count)
        def _(index):
            j = half - 1 - index
            for c in range(CORES):
                returned(hosted, j, c).wait_recv()
            for r in range(tokens // block):
                total[r * block:(r + 1) * block, :] += mixed(hosted * half + j, r)

    for c in range(CORES):
        returned(1, 1, c).wait_recv()
    for r in range(tokens // block):
        rows = slice(r * block, (r + 1) * block)
        out_ref[rows, :] = (total[rows, :] + mixed(half + 1, r)).astype(jnp.bfloat16)

    for hosted in range(2):
        forward(hosted, 0, 1 - core).wait_send()
        reply(hosted, 0, 1 - core).wait_send()

        @pl.loop(1, half)
        def _(j):
            for c in range(CORES):
                forward(hosted, j, c).wait_send()
                reply(hosted, j, c).wait_send()
    for array in range(2):
        lend(array).wait_send()
        for phase in range(2):
            for k in range(span if phase == 1 else 1):
                for shift in range(1, span):
                    share(array, phase, k, shift).wait_send()


def solution(mesh):
    n = mesh.shape["ep"]
    chips = n // CORES
    groups = mesh.shape["dp"]
    span = math.isqrt(groups)

    def local_layer(tokens, w_gate, expert_ids, keep_second, w_in, w_out):
        count, model = tokens.shape[1:]
        experts = w_gate.shape[1]
        hid = w_in.shape[2]
        capacity = 2 * count // experts
        buffer = pltpu.VMEM((chips, CORES, capacity, model), jnp.bfloat16)
        vmem = pl.BlockSpec(memory_space=pltpu.VMEM)
        hbm = pl.BlockSpec(memory_space=pltpu.HBM)
        out = pl.pallas_call(
            functools.partial(layer_kernel, n, groups),
            out_shape=pltpu.VMEM((count, model), jnp.bfloat16),
            in_specs=[hbm] * 6,
            out_specs=vmem,
            scratch_shapes=[
                pltpu.VMEM((count, model), jnp.bfloat16),
                pltpu.VMEM((experts, model), jnp.bfloat16),
                pltpu.VMEM((2, count), jnp.int32),
                pltpu.VMEM((1, count), jnp.int32),
                pltpu.VMEM((model, hid), jnp.bfloat16),
                pltpu.VMEM((hid, model), jnp.bfloat16),
                pltpu.VMEM((model, hid), jnp.bfloat16),
                pltpu.VMEM((hid, model), jnp.bfloat16),
                buffer, buffer, buffer, buffer,
                pltpu.VMEM((CORES * capacity, hid), jnp.bfloat16),
                pltpu.VMEM((chips, count, CORES * capacity), jnp.bfloat16),
                pltpu.VMEM((count, model), jnp.float32),
                pltpu.VMEM((8, count), jnp.int32),
                pltpu.SemaphoreType.DMA((6,)),
                pltpu.SemaphoreType.DMA((chips, CORES)),
                pltpu.SemaphoreType.DMA((chips, CORES)),
                pltpu.SemaphoreType.DMA((chips, CORES)),
                pltpu.SemaphoreType.DMA((chips, CORES)),
                pltpu.SemaphoreType.DMA((2,)),
                pltpu.SemaphoreType.DMA((2, 2, span, span)),
                pltpu.SemaphoreType.DMA((2, groups)),
                pltpu.SemaphoreType.REGULAR((chips // 2,)),
            ],
            compiler_params=pltpu.CompilerParams(collective_id=0, has_side_effects=True, vmem_limit_bytes=54 * 2**20),
        )(*(pltpu.with_memory_space_constraint(x, pltpu.HBM) for x in (tokens[0], w_gate.T, expert_ids[0].T, keep_second, w_in[0], w_out[0])))
        return out[None]

    group_spec = P(("dp", "ep"))
    return jax.shard_map(local_layer, mesh=mesh, in_specs=(group_spec, P(), group_spec, group_spec, P("ep"), P("ep")), out_specs=group_spec, check_vma=False)
```

```python
import functools
import math

import jax
import jax.numpy as jnp
from jax import lax
from jax.experimental import pallas as pl
from jax.experimental.pallas import tpu as pltpu
from jax.sharding import PartitionSpec as P

MESH = pl.DeviceIdType.MESH
CORES = 2
LANES = 128


def route_slots(ids_ref, keep_ref, experts, capacity):
    tokens = ids_ref.shape[1]
    first = ids_ref[0:1, :]
    second = ids_ref[1:2, :]
    keep = keep_ref[0:1, :]
    expert_row = lax.broadcasted_iota(jnp.int32, (experts, tokens), 0)
    first_hot = jnp.where(expert_row == first, 1.0, 0.0)
    second_hot = jnp.where((expert_row == second) & (keep == 1), 1.0, 0.0)
    hot = jnp.concatenate([first_hot, second_hot], axis=0)
    blocks = tokens // LANES
    stacked = jnp.concatenate([hot[:, b * LANES:(b + 1) * LANES] for b in range(blocks)], axis=0).astype(jnp.bfloat16)
    row = lax.broadcasted_iota(jnp.int32, (LANES, 2 * LANES), 0)
    col = lax.broadcasted_iota(jnp.int32, (LANES, 2 * LANES), 1)
    before = jnp.where((row < col) | (col >= LANES), 1.0, 0.0).astype(jnp.bfloat16)
    counts = jnp.dot(stacked, before, preferred_element_type=jnp.float32)
    rows = 2 * experts
    offset = jnp.zeros((rows, LANES), jnp.float32)
    prefix = []
    for b in range(blocks):
        part = counts[b * rows:(b + 1) * rows]
        prefix.append(part[:, :LANES] + offset)
        offset = offset + part[:, LANES:]
    first_total = offset[:experts]
    slot_first, slot_second = [], []
    for b in range(blocks):
        lanes = slice(b * LANES, (b + 1) * LANES)
        pos_first = jnp.sum(prefix[b][:experts] * first_hot[:, lanes], axis=0, keepdims=True)
        pos_second = jnp.sum((prefix[b][experts:] + first_total) * second_hot[:, lanes], axis=0, keepdims=True)
        slot_first.append(pos_first)
        slot_second.append(pos_second)
    pos_first = jnp.concatenate(slot_first, axis=1).astype(jnp.int32)
    pos_second = jnp.concatenate(slot_second, axis=1).astype(jnp.int32)
    slot_first = jnp.where(pos_first < capacity, first * capacity + pos_first, -1)
    slot_second = jnp.where((keep == 1) & (pos_second < capacity), second * capacity + pos_second, -1)
    return slot_first, slot_second, first_hot, second_hot


def layer_kernel(n, groups, tokens_hbm, gate_hbm, ids_hbm, keep_hbm, w_in_hbm, w_out_hbm, out_ref,
                 tokens_ref, gate_ref, ids_ref, keep_ref, w_in, w_out, host_in, host_out, send, recv, back, ret, hidden, combine, total, slots,
                 load_sem, send_sem, recv_sem, back_sem, ret_sem, lend_sem, share_sem, slice_sem, reach_sem):
    me = lax.axis_index("ep")
    part = lax.axis_index("dp")
    chips = n // CORES
    half = chips // 2
    chip = me // CORES
    core = lax.rem(me, CORES)
    side = 1 - 2 * core
    experts = gate_ref.shape[0]
    tokens, model = tokens_ref.shape
    hid = w_in.shape[1]
    capacity = 2 * tokens // experts
    pair = CORES * capacity
    span = math.isqrt(groups)
    part_x = part // span
    part_y = lax.rem(part, span)

    load_ids = pltpu.make_async_copy(ids_hbm, ids_ref, load_sem.at[0])
    load_keep = pltpu.make_async_copy(keep_hbm, keep_ref, load_sem.at[1])
    load_gate = pltpu.make_async_copy(gate_hbm, gate_ref, load_sem.at[2])
    load_tokens = pltpu.make_async_copy(tokens_hbm, tokens_ref, load_sem.at[3])
    load_in = pltpu.make_async_copy(w_in_hbm, w_in, load_sem.at[4])
    load_out = pltpu.make_async_copy(w_out_hbm, w_out, load_sem.at[5])
    load_ids.start()
    load_keep.start()
    load_tokens.start()
    load_gate.start()

    def share_peer(array, phase, shift):
        if (array == 0) == (phase == 0):
            return lax.rem(part_x + shift, span) * span + part_y
        return part_x * span + lax.rem(part_y + shift, span)

    barrier = pltpu.get_barrier_semaphore()
    ahead, behind, partner = lax.rem(me + CORES, n), lax.rem(me + n - CORES, n), me + 1 - 2 * core
    for near in (ahead, behind, partner):
        pl.semaphore_signal(barrier, inc=1, device_id=(part, near), device_id_type=MESH)
    for phase in range(2):
        for shift in range(1, span):
            pl.semaphore_signal(barrier, inc=1, device_id=(share_peer(0, phase, shift), me), device_id_type=MESH)


    def wrap(value):
        return lax.rem(value + chips, chips)

    def run_chip(hosted, j, c):
        sign = 1 - 2 * c
        return wrap(chip + sign * j) if hosted else wrap(chip - sign * j)

    def expert_of(hosted, j, c):
        sign = 1 - 2 * c
        return (wrap(run_chip(hosted, j, c) + sign) if hosted else run_chip(hosted, j, c)) * CORES + c

    def source_chip(hosted, j):
        return wrap(chip - side * j) if hosted else wrap(chip + side * j)

    def forward(hosted, j, c):
        step = hosted * half + j
        return pltpu.make_async_remote_copy(
            src_ref=send.at[step, c], dst_ref=recv.at[step, core],
            send_sem=send_sem.at[step, c], recv_sem=recv_sem.at[step, core],
            device_id=(part, run_chip(hosted, j, c) * CORES + c), device_id_type=MESH)

    def arrived(hosted, j, c):
        step = hosted * half + j
        return pltpu.make_async_remote_copy(
            src_ref=send.at[step, c], dst_ref=recv.at[step, c],
            send_sem=send_sem.at[step, c], recv_sem=recv_sem.at[step, c],
            device_id=(part, run_chip(hosted, j, c) * CORES + c), device_id_type=MESH)

    def reply(hosted, j, c):
        step = hosted * half + j
        return pltpu.make_async_remote_copy(
            src_ref=back.at[step, c], dst_ref=ret.at[step, core],
            send_sem=back_sem.at[step, c], recv_sem=ret_sem.at[step, core],
            device_id=(part, source_chip(hosted, j) * CORES + c), device_id_type=MESH)

    def returned(hosted, j, c):
        step = hosted * half + j
        return pltpu.make_async_remote_copy(
            src_ref=back.at[step, c], dst_ref=ret.at[step, c],
            send_sem=back_sem.at[step, c], recv_sem=ret_sem.at[step, c],
            device_id=(part, source_chip(hosted, j) * CORES + c), device_id_type=MESH)

    own_hbm = (w_in_hbm, w_out_hbm)
    host = (host_in, host_out)

    def slice_of(array, owner):
        rows = host[array].shape[0] // groups
        return pl.ds(pl.multiple_of(owner * rows, rows), rows)

    def lend(array):
        return pltpu.make_async_remote_copy(
            src_ref=own_hbm[array].at[slice_of(array, part)], dst_ref=host[array].at[slice_of(array, part)],
            send_sem=lend_sem.at[array], recv_sem=slice_sem.at[array, part],
            device_id=(part, wrap(chip - side) * CORES + core), device_id_type=MESH)

    pl.semaphore_wait(barrier, 3 + 2 * (span - 1))
    lend(0).start()
    lend(1).start()
    for level in range(half - 1):
        for near in (ahead, behind):
            pl.semaphore_signal(reach_sem.at[level], inc=1, device_id=(part, near), device_id_type=MESH)
        pl.semaphore_wait(reach_sem.at[level], 2)
    pl.semaphore_signal(reach_sem.at[half - 1], inc=1, device_id=(part, partner), device_id_type=MESH)
    pl.semaphore_wait(reach_sem.at[half - 1], 1)

    load_ids.wait()
    load_keep.wait()
    slot_first, slot_second, first_hot, second_hot = route_slots(ids_ref, keep_ref, experts, capacity)
    slots[0:1, :] = slot_first
    slots[1:2, :] = slot_second

    def slice_owner(array, shift):
        return share_peer(array, 0, shift)

    def share(array, phase, k, shift):
        owner = slice_owner(array, k)
        return pltpu.make_async_remote_copy(
            src_ref=host[array].at[slice_of(array, owner)], dst_ref=host[array].at[slice_of(array, owner)],
            send_sem=share_sem.at[array, phase, k, shift], recv_sem=slice_sem.at[array, owner],
            device_id=(share_peer(array, phase, shift), me), device_id_type=MESH)

    def slice_ready(array, owner):
        return pltpu.make_async_remote_copy(
            src_ref=host[array].at[slice_of(array, owner)], dst_ref=host[array].at[slice_of(array, owner)],
            send_sem=lend_sem.at[array], recv_sem=slice_sem.at[array, owner],
            device_id=(share_peer(0, 0, 1), me), device_id_type=MESH)

    slot_row = lax.broadcasted_iota(jnp.int32, (capacity, tokens), 0)

    def pick_of(hosted, j):
        halves = []
        for c in range(CORES):
            base = expert_of(hosted, j, c) * capacity
            hit = (slot_row == slots[0:1, :] - base) | (slot_row == slots[1:2, :] - base)
            halves.append(jnp.where(hit, 1.0, 0.0))
        return jnp.concatenate(halves, axis=0).astype(jnp.bfloat16)

    def dispatch(hosted, j):
        rows = jnp.dot(pick_of(hosted, j), tokens_ref[...], preferred_element_type=jnp.float32).astype(jnp.bfloat16)
        send[hosted * half + j] = rows.reshape(CORES, capacity, model)

    load_tokens.wait()
    load_in.start()
    load_out.start()
    far_first = range(half - 1, 0, -1)
    for hosted in range(2):
        for j in (*far_first, 0):
            dispatch(hosted, j)
    for hosted in range(2):
        forward(hosted, 0, 1 - core).start()
        recv[hosted * half, core] = send[hosted * half, core]

    load_gate.wait()
    logits = lax.dot_general(gate_ref[...], tokens_ref[...], (((1,), (1,)), ((), ())), preferred_element_type=jnp.float32)
    shifted = jnp.exp(logits - jnp.max(logits, axis=0, keepdims=True))
    probs = shifted / jnp.sum(shifted, axis=0, keepdims=True)
    gate_first = jnp.sum(probs * first_hot, axis=0, keepdims=True)
    gate_second = jnp.sum(probs * second_hot, axis=0, keepdims=True)
    gate_total = gate_first + gate_second
    gate_first = gate_first / gate_total
    gate_second = gate_second / gate_total
    for hosted in range(2):
        for j in range(half):
            weights = []
            for c in range(CORES):
                base = expert_of(hosted, j, c) * capacity
                weights.append(jnp.where(slot_row == slots[0:1, :] - base, gate_first, 0.0) + jnp.where(slot_row == slots[1:2, :] - base, gate_second, 0.0))
            combine[hosted * half + j] = jnp.concatenate(weights, axis=0).astype(jnp.bfloat16).T

    load_in.wait()
    load_out.wait()

    def experts_on(hosted, j):
        step = hosted * half + j
        up_ref, down_ref = (host_in, host_out) if hosted else (w_in, w_out)
        rows = recv[step].reshape(pair, model)
        tile = 512
        for t in range(hid // tile):
            cols = slice(t * tile, (t + 1) * tile)
            up = jnp.dot(rows, up_ref[:, cols], preferred_element_type=jnp.float32)
            hidden[:, cols] = jnp.maximum(up, 0.0).astype(jnp.bfloat16)
        tile = 256
        for t in range(model // tile):
            cols = slice(t * tile, (t + 1) * tile)
            down = jnp.dot(hidden[...], down_ref[:, cols], preferred_element_type=jnp.float32).astype(jnp.bfloat16)
            for c in range(CORES):
                back[step, c, :, cols] = down[c * capacity:(c + 1) * capacity]

    def local_experts(hosted):
        arrived(hosted, 0, 1 - core).wait_recv()
        experts_on(hosted, 0)
        reply(hosted, 0, 1 - core).start()
        ret[hosted * half, core] = back[hosted * half, core]

    def remote_experts(hosted):
        @pl.loop(0, half - 1)
        def _(index):
            j = half - 1 - index
            for c in range(CORES):
                arrived(hosted, j, c).wait_recv()
            experts_on(hosted, j)
            for c in (1, 0):
                reply(hosted, j, c).start()

    def first_share(array):
        slice_ready(array, part).wait_recv()
        for shift in range(1, span):
            share(array, 0, 0, shift).start()
        for shift in range(1, span):
            share(array, 1, 0, shift).start()

    def second_share(array):
        for k in range(1, span):
            slice_ready(array, slice_owner(array, k)).wait_recv()
            for shift in range(1, span):
                share(array, 1, k, shift).start()

    first_share(0)
    local_experts(0)
    first_share(1)
    for hosted in range(2):
        for j in far_first:
            for c in (core, 1 - core):
                forward(hosted, j, c).start()
    second_share(0)
    remote_experts(0)
    second_share(1)
    for array in range(2):
        for k in range(span):
            for shift in range(1, span):
                owner = share_peer(0, 0, k) // span * span + lax.rem(part_y + shift, span) if array == 0 else lax.rem(part_x + shift, span) * span + lax.rem(part_y + k, span)
                slice_ready(array, owner).wait_recv()
    remote_experts(1)
    local_experts(1)

    block = 256

    def mixed(step, r):
        return jnp.dot(combine[step, r * block:(r + 1) * block, :], ret[step].reshape(pair, model), preferred_element_type=jnp.float32)

    for hosted in range(2):
        returned(hosted, 0, 1 - core).wait_recv()
        for r in range(tokens // block):
            rows = slice(r * block, (r + 1) * block)
            if hosted == 0:
                total[rows, :] = mixed(0, r)
            else:
                total[rows, :] += mixed(half, r)
        count = half - 1 if hosted == 0 else half - 2

        @pl.loop(0, count)
        def _(index):
            j = half - 1 - index
            for c in range(CORES):
                returned(hosted, j, c).wait_recv()
            for r in range(tokens // block):
                total[r * block:(r + 1) * block, :] += mixed(hosted * half + j, r)

    for c in range(CORES):
        returned(1, 1, c).wait_recv()
    for r in range(tokens // block):
        rows = slice(r * block, (r + 1) * block)
        out_ref[rows, :] = (total[rows, :] + mixed(half + 1, r)).astype(jnp.bfloat16)

    for hosted in range(2):
        forward(hosted, 0, 1 - core).wait_send()
        reply(hosted, 0, 1 - core).wait_send()

        @pl.loop(1, half)
        def _(j):
            for c in range(CORES):
                forward(hosted, j, c).wait_send()
                reply(hosted, j, c).wait_send()
    for array in range(2):
        lend(array).wait_send()
        for phase in range(2):
            for k in range(span if phase == 1 else 1):
                for shift in range(1, span):
                    share(array, phase, k, shift).wait_send()


def solution(mesh):
    n = mesh.shape["ep"]
    chips = n // CORES
    groups = mesh.shape["dp"]
    span = math.isqrt(groups)

    def local_layer(tokens, w_gate, expert_ids, keep_second, w_in, w_out):
        count, model = tokens.shape[1:]
        experts = w_gate.shape[1]
        hid = w_in.shape[2]
        capacity = 2 * count // experts
        buffer = pltpu.VMEM((chips, CORES, capacity, model), jnp.bfloat16)
        vmem = pl.BlockSpec(memory_space=pltpu.VMEM)
        hbm = pl.BlockSpec(memory_space=pltpu.HBM)
        out = pl.pallas_call(
            functools.partial(layer_kernel, n, groups),
            out_shape=pltpu.VMEM((count, model), jnp.bfloat16),
            in_specs=[hbm] * 6,
            out_specs=vmem,
            scratch_shapes=[
                pltpu.VMEM((count, model), jnp.bfloat16),
                pltpu.VMEM((experts, model), jnp.bfloat16),
                pltpu.VMEM((2, count), jnp.int32),
                pltpu.VMEM((1, count), jnp.int32),
                pltpu.VMEM((model, hid), jnp.bfloat16),
                pltpu.VMEM((hid, model), jnp.bfloat16),
                pltpu.VMEM((model, hid), jnp.bfloat16),
                pltpu.VMEM((hid, model), jnp.bfloat16),
                buffer, buffer, buffer, buffer,
                pltpu.VMEM((CORES * capacity, hid), jnp.bfloat16),
                pltpu.VMEM((chips, count, CORES * capacity), jnp.bfloat16),
                pltpu.VMEM((count, model), jnp.float32),
                pltpu.VMEM((8, count), jnp.int32),
                pltpu.SemaphoreType.DMA((6,)),
                pltpu.SemaphoreType.DMA((chips, CORES)),
                pltpu.SemaphoreType.DMA((chips, CORES)),
                pltpu.SemaphoreType.DMA((chips, CORES)),
                pltpu.SemaphoreType.DMA((chips, CORES)),
                pltpu.SemaphoreType.DMA((2,)),
                pltpu.SemaphoreType.DMA((2, 2, span, span)),
                pltpu.SemaphoreType.DMA((2, groups)),
                pltpu.SemaphoreType.REGULAR((chips // 2,)),
            ],
            compiler_params=pltpu.CompilerParams(collective_id=0, has_side_effects=True, vmem_limit_bytes=54 * 2**20),
        )(*(pltpu.with_memory_space_constraint(x, pltpu.HBM) for x in (tokens[0], w_gate.T, expert_ids[0].T, keep_second, w_in[0], w_out[0])))
        return out[None]

    group_spec = P(("dp", "ep"))
    return jax.shard_map(local_layer, mesh=mesh, in_specs=(group_spec, P(), group_spec, group_spec, P("ep"), P("ep")), out_specs=group_spec, check_vma=False)
```
